32 devices in a mesh: query: 2 (over y), ctx: 16 (over z, x, core).
Axes of the slice: x: 2, y: 2, z: 4, core: 2. Of those that a mesh axis runs over, the one named last changes fastest.
Arguments:
- query_states: bfloat16 [64, 3072], P('query'), may hold values from -370 to 370
- key_states: bfloat16 [16384, 3072], P('ctx', 'query'), may hold values from -10.5 to 10.5
- value_states: bfloat16 [16384, 3072], P('ctx', 'query'), may hold values from -6 to 6
- level_ids: int32 [16384], P('ctx'), may hold values from 0 to 4, as said below
- level_bias: float32 [5, 24], replicated, may hold values from -1.5 to 1.5
- live_counts: int32 [16], P('ctx'), may hold values from 256 to 1024, as said below
- out_grad: bfloat16 [64, 3072], P('query'), may hold values from -6 to 6
Outputs:
- attn_out: bfloat16 [64, 3072], P(('query', 'ctx'))
- query_grad: bfloat16 [64, 3072], P(('query', 'ctx'))
- key_grad: bfloat16 [16384, 3072], P('ctx', 'query')
- value_grad: bfloat16 [16384, 3072], P('ctx', 'query')
The draws below stay inside these ranges and needn't reach their ends.
Inputs may be any that keep to these rules, and one draw needn't show every extreme that they name: Owner c's slots c * 1024 to c * 1024 + live_counts[c] - 1 are live, its other slots are empty; at least one owner has all 1024 slots live. `level_ids`: constant over each aligned run of 16 slots.
All inputs are finite; a program needn't handle non-finite values.
Results may differ from the reference program's by a relative error of at most 0.012.
Values may be sent and summed in bfloat16 or wider, within the bound.
No kernel may reach another device: no remote copies, remote signals or barrier semaphores. Data moves between devices by JAX's collectives and lax.ppermute only.
A program may use at most 64 MiB of HBM per device.

```python
import math
import jax
import jax.numpy as jnp
from jax import lax

HEADS = 24
HEAD_DIM = 128
WIDTH = 3072
LEVELS = 5
FRAME_SLOTS = 16
QDEV = 32
CDEV = 1024
NQ = 64
NC = 16384
OWNERS = 16
N_QUERY = 2


def shared_keys(key):
    base = jnp.clip(jax.random.normal(jax.random.fold_in(key, 101), (NC, WIDTH), jnp.float32), -5.0, 5.0)
    return base


def draw_key_states(key, part):
    return shared_keys(key).astype(jnp.bfloat16)


def draw_query_states(key, part):
    queries = jnp.clip(jax.random.normal(jax.random.fold_in(key, 111), (NQ, WIDTH), jnp.float32), -5.0, 5.0)
    return queries.astype(jnp.bfloat16)


def draw_level_ids(key, part):
    frame_levels = jax.random.randint(jax.random.fold_in(key, 201), (NC // FRAME_SLOTS,), 0, LEVELS, jnp.int32)
    return jnp.repeat(frame_levels, FRAME_SLOTS)


def draw_live_counts(key, part):
    counts = jax.random.randint(jax.random.fold_in(key, 301), (OWNERS,), CDEV // 4, CDEV + 1, jnp.int32)
    full_owner = jax.random.randint(jax.random.fold_in(key, 302), (), 0, OWNERS, jnp.int32)
    owner_index = lax.iota(jnp.int32, OWNERS)
    return jnp.where(owner_index == full_owner, CDEV, counts).astype(jnp.int32)


def steps_of(key, shape, cuts, least, largest):
    def one(position, blocks):
        steps = jax.random.uniform(jax.random.fold_in(jax.random.fold_in(key, 6), position), (blocks,), jnp.float32, least / len(cuts), largest / len(cuts))
        return jnp.repeat(jnp.exp(steps), shape[position] // blocks).reshape((-1,) + (1,) * (len(shape) - position - 1))

    level = one(*cuts[0])
    for cut in cuts[1:]:
        level = level * one(*cut)
    return level


def bell_draw(own_key, shape, scale, reach, pieces=(), held_as=jnp.bfloat16):
    result = scale * jax.random.normal(own_key, shape, jnp.float32)
    if pieces:
        result = result * steps_of(own_key, shape, pieces, -0.22, 0.18)
    return jnp.clip(result, -reach, reach).astype(held_as)


def setup_inputs(seed: int = 0) -> dict:
    streams_of = jax.random.split(jax.random.key(seed), 8)
    return {
        "query_states": draw_query_states(jax.random.fold_in(streams_of[7], 71), 0),
        "key_states": draw_key_states(jax.random.fold_in(streams_of[7], 71), 0),
        "value_states": bell_draw(streams_of[2], (NC, WIDTH), 1.0, 6.0, ((0, 16), (1, 2))),
        "level_ids": draw_level_ids(jax.random.fold_in(streams_of[7], 71), 0),
        "level_bias": jnp.clip(jax.random.uniform(streams_of[4], (LEVELS, HEADS), jnp.float32, -1.5, 1.5), -1.5, 1.5),
        "live_counts": draw_live_counts(jax.random.fold_in(streams_of[7], 71), 0),
        "out_grad": bell_draw(streams_of[6], (NQ, WIDTH), 1.0, 6.0, ((0, 2),)),
    }


def reference(query_states, key_states, value_states, level_ids, level_bias, live_counts, out_grad):
    softmax_scale = 1.0 / math.sqrt(HEAD_DIM)
    level_term = level_bias[level_ids]
    slot_index = jnp.arange(NC, dtype=jnp.int32)
    live_slots = slot_index % CDEV < jnp.repeat(live_counts, CDEV)
    key_heads = key_states.astype(jnp.float32).reshape(NC, HEADS, HEAD_DIM)
    value_heads = value_states.astype(jnp.float32).reshape(NC, HEADS, HEAD_DIM)
    value_blocks = value_heads.reshape(OWNERS, CDEV, HEADS, HEAD_DIM)
    query_blocks = query_states.reshape(N_QUERY, QDEV, HEADS, HEAD_DIM)
    grad_blocks = out_grad.reshape(N_QUERY, QDEV, HEADS, HEAD_DIM)

    def query_block(carry, blocks):
        block_queries, block_grads = blocks
        queries = block_queries.astype(jnp.float32)
        grad_heads = block_grads.astype(jnp.float32)
        scores = jnp.einsum('qhd,khd->hqk', queries, key_heads) * softmax_scale + level_term.T[:, None, :]
        scores = jnp.where(live_slots[None, None, :], scores, -1e+30)
        grouped = scores.reshape(HEADS, QDEV, OWNERS, CDEV)
        block_max = lax.optimization_barrier(jnp.max(grouped, axis=3))
        raw_weights = jnp.exp(grouped - block_max[..., None])
        block_sum = lax.optimization_barrier(jnp.sum(raw_weights, axis=3))
        rounded = lax.optimization_barrier(raw_weights.astype(jnp.bfloat16)).astype(jnp.float32)
        block_out = jnp.einsum('hqck,ckhd->hqcd', rounded, value_blocks)
        row_max = lax.optimization_barrier(jnp.max(block_max, axis=2))
        factor = jnp.exp(block_max - row_max[..., None])
        total = lax.optimization_barrier(jnp.sum(factor * block_sum, axis=2))
        attention = lax.optimization_barrier(jnp.sum(factor[..., None] * block_out, axis=2)) / total[..., None]
        log_total = row_max + jnp.log(total)
        deltas = lax.optimization_barrier(jnp.sum(jnp.transpose(grad_heads, (1, 0, 2)) * attention, axis=2))
        probabilities = jnp.exp(scores - log_total[..., None])
        dprobs = jnp.einsum('qhd,khd->hqk', grad_heads, value_heads)
        dscores = lax.optimization_barrier((probabilities * (dprobs - deltas[..., None])).astype(jnp.bfloat16)).astype(jnp.float32)
        prob_rounded = lax.optimization_barrier(probabilities.astype(jnp.bfloat16)).astype(jnp.float32)
        key_part = softmax_scale * jnp.einsum('hqk,qhd->khd', dscores, queries)
        value_part = jnp.einsum('hqk,qhd->khd', prob_rounded, grad_heads)
        query_part = softmax_scale * jnp.einsum('hqk,khd->qhd', dscores, key_heads)
        key_sum, value_sum = carry
        key_sum = key_sum + lax.optimization_barrier(key_part.reshape(NC, WIDTH).astype(jnp.bfloat16)).astype(jnp.float32)
        value_sum = value_sum + lax.optimization_barrier(value_part.reshape(NC, WIDTH).astype(jnp.bfloat16)).astype(jnp.float32)
        attn_rows = jnp.transpose(attention, (1, 0, 2)).reshape(QDEV, WIDTH)
        return ((key_sum, value_sum), (attn_rows, query_part.reshape(QDEV, WIDTH)))
    start = (jnp.zeros((NC, WIDTH), jnp.float32), jnp.zeros((NC, WIDTH), jnp.float32))
    sums, stacked = lax.scan(query_block, start, (query_blocks, grad_blocks))
    attn_out = stacked[0].reshape(NQ, WIDTH).astype(jnp.bfloat16)
    query_grad = stacked[1].reshape(NQ, WIDTH).astype(jnp.bfloat16)
    return (attn_out, query_grad, sums[0].astype(jnp.bfloat16), sums[1].astype(jnp.bfloat16))
```

```python
import functools
import math

import jax
import jax.numpy as jnp
from jax import lax
from jax.experimental import pallas as pl
from jax.experimental.pallas import tpu as pltpu
from jax.sharding import PartitionSpec as P

F32 = jnp.float32
BF16 = jnp.bfloat16
MIB = 1024 * 1024
VMEM = pl.BlockSpec(memory_space=pltpu.VMEM)


def call(body, out_shape, vmem_mib, flops, **kwargs):
    return pl.pallas_call(
        body,
        out_shape=out_shape,
        compiler_params=pltpu.CompilerParams(vmem_limit_bytes=vmem_mib * MIB),
        cost_estimate=pl.CostEstimate(flops=flops, bytes_accessed=MIB, transcendentals=0),
        **kwargs,
    )


def nt(a, b):
    return lax.dot_general(a, b, (((1,), (1,)), ((), ())), preferred_element_type=F32)


def nn(a, b):
    return lax.dot_general(a, b, (((1,), (0,)), ((), ())), preferred_element_type=F32)


class Plan:
    def __init__(self, query_states, key_states, level_bias):
        self.query_ways = lax.axis_size("query")
        self.owner_ways = lax.axis_size("ctx")
        self.slots, self.features = key_states.shape
        self.heads = level_bias.shape[1] // self.query_ways
        self.head_size = self.features // self.heads
        self.scale = 1.0 / math.sqrt(self.head_size)
        self.own_rows = query_states.shape[0]
        self.rows = self.own_rows * self.query_ways
        self.part_rows = self.own_rows // self.owner_ways
        self.last_rows = self.part_rows * self.query_ways
        self.group = 2 if self.heads % 2 == 0 and self.rows <= 128 else 1
        self.groups = self.heads // self.group
        self.lanes = self.group * self.rows
        self.rounds = self.owner_ways.bit_length() - 1
        assert 1 << self.rounds == self.owner_ways and self.groups <= 8
        counts = [self.rows]
        for _ in range(self.rounds):
            half = counts[-1] // 2
            counts.append(half if half >= 8 else counts[-1])
        self.counts = counts

    def split(self, k):
        return k < self.rounds and self.counts[k + 1] < self.counts[k]

    def bit(self, k):
        return (lax.axis_index("ctx") >> k) & 1

    def keep(self, k):
        return self.bit(k) * self.counts[k + 1] if self.split(k) else 0

    def give(self, k):
        return (1 - self.bit(k)) * self.counts[k + 1] if self.split(k) else 0

    def base(self, k):
        return sum((self.keep(j) for j in range(k)), 0)

    def last_offset(self):
        offset = 0
        for k in range(self.rounds):
            if not self.split(k):
                offset = offset + self.bit(k) * (self.rows >> (k + 1))
        return offset


def aligned(x, by):
    return pl.multiple_of(x, by) if by >= 8 and not isinstance(x, int) else x


def forward_body(plan, split_parts, *refs):
    if split_parts:
        q_ref, g_ref, moved_ref = refs[:3]
        refs = refs[3:]
    else:
        moved_ref = refs[0]
        refs = refs[1:]
    (k_ref, v_ref, term_ref, part_ref, send_ref, stat_ref, pair_ref, qb_ref, gb_ref) = refs[:9]
    source, scores, dprobs, columns = refs[9:]
    rows, size, group = plan.rows, plan.head_size, plan.group
    width = group * size
    place = lax.broadcasted_iota(jnp.int32, (rows, rows), 0)
    column = lax.broadcasted_iota(jnp.int32, (rows, rows), 1)
    inner = place % plan.last_rows
    outer = place // plan.last_rows
    owner = jnp.zeros_like(outer)
    for k in range(plan.rounds):
        owner = owner | (((outer >> (plan.rounds - 1 - k)) & 1) << k)
    wanted = (
        inner // plan.part_rows * plan.own_rows + owner * plan.part_rows + inner % plan.part_rows
    )
    permute = (column == wanted).astype(F32).astype(BF16)
    qb_ref[...] = jnp.zeros_like(qb_ref)
    gb_ref[...] = jnp.zeros_like(gb_ref)
    for which, own_ref, block_ref in ((0, 0, qb_ref), (1, 1, gb_ref)):
        if split_parts:
            mine = (q_ref, g_ref)[own_ref]
            start = pl.multiple_of(lax.axis_index("query") * plan.features, 128)
            source[: plan.own_rows] = mine[:, pl.ds(start, plan.features)]
            source[plan.own_rows :] = moved_ref[which]
        else:
            source[...] = moved_ref[which]
        for p in range(plan.groups):
            ordered = nn(permute, source[:, p * width : (p + 1) * width]).astype(BF16)
            for q in range(group):
                block_ref[p, q * rows : (q + 1) * rows, q * size : (q + 1) * size] = ordered[
                    :, q * size : (q + 1) * size
                ]
    columns[...] = jnp.zeros_like(columns)
    step = 16
    for p in range(plan.groups):
        keys = k_ref[:, p * width : (p + 1) * width]
        values = v_ref[:, p * width : (p + 1) * width]
        scores[...] = nt(qb_ref[p], keys)
        dprobs[...] = nt(gb_ref[p], values)
        for r in range(0, plan.lanes, step):
            h = p * group + r // rows
            s = scores[r : r + step] * plan.scale + term_ref[h : h + 1, :]
            top = jnp.max(s, axis=1, keepdims=True)
            e = jnp.exp(s - top)
            total = jnp.sum(e, axis=1, keepdims=True)
            d = dprobs[r : r + step]
            mean = jnp.sum(e * d, axis=1, keepdims=True) / total
            pair_ref[p, r : r + step, :] = e.astype(BF16)
            pair_ref[p, plan.lanes + r : plan.lanes + r + step, :] = (e * (d - mean)).astype(BF16)
            columns[r : r + step, p : p + 1] = top
            columns[r : r + step, 8 + p : 9 + p] = total
            columns[r : r + step, 16 + p : 17 + p] = mean
        with_values = nn(pair_ref[p, : plan.lanes, :], values)
        with_keys = nn(pair_ref[p], keys)
        for q in range(group):
            at = slice(q * rows, (q + 1) * rows)
            of = slice(q * size, (q + 1) * size)
            part_ref[0, p * group + q] = with_values[at, of]
            part_ref[1, p * group + q] = with_keys[at, of]
            part_ref[2, p * group + q] = with_keys[plan.lanes + q * rows : plan.lanes + (q + 1) * rows, of]
    count = plan.counts[1]
    gone = pl.ds(aligned(plan.give(0), count), count)
    for a in range(3):
        for h in range(plan.heads):
            send_ref[a, h] = part_ref[a, h, gone, :].astype(BF16)
    stat_ref[...] = columns[...].T[:24]


def merge_body(plan, k, part_ref, came_ref, stat_ref, stat_came_ref, *refs):
    last = k == plan.rounds - 1
    if last:
        stat_new_ref, own_ref, send_ref, table = refs
    else:
        part_new_ref, send_ref, stat_new_ref, table = refs
    top1, total1, mean1 = (stat_ref[8 * t : 8 * t + 8] for t in range(3))
    top2, total2, mean2 = (stat_came_ref[8 * t : 8 * t + 8] for t in range(3))
    top = jnp.maximum(top1, top2)
    f1 = jnp.exp(top1 - top)
    f2 = jnp.exp(top2 - top)
    total = f1 * total1 + f2 * total2
    live = total > 0.0
    inverse = 1.0 / jnp.where(live, total, 1.0)
    w1 = f1 * total1 * inverse
    w2 = f2 * total2 * inverse
    stat_new_ref[0:8] = top
    stat_new_ref[8:16] = total
    stat_new_ref[16:24] = mean1 * w1 + mean2 * w2
    gap = mean1 - mean2
    rest = 128 - 40
    table[...] = jnp.concatenate(
        [f1, f2, f1 * w2 * gap, -f2 * w1 * gap, inverse, jnp.zeros((rest, plan.lanes), F32)], axis=0
    ).T
    count = plan.counts[k + 1]
    kept = pl.ds(aligned(plan.keep(k), count), count)
    base = plan.base(k + 1)
    if last:
        offset = plan.last_offset()
    for h in range(plan.heads):
        p, q = h // plan.group, h % plan.group
        at = pl.ds(aligned(q * plan.rows + base, count), count)
        factors = table[at, :]
        col = lambda t: factors[:, 8 * t + p : 8 * t + p + 1]
        out1, key1, dif1 = (part_ref[a, h, kept, :] for a in range(3))
        out2, key2, dif2 = (came_ref[a, h].astype(F32) for a in range(3))
        c1, c2 = col(0), col(1)
        out = c1 * out1 + c2 * out2
        dif = c1 * dif1 + c2 * dif2 + col(2) * key1 + col(3) * key2
        if not last:
            part_new_ref[0, h] = out
            part_new_ref[1, h] = c1 * key1 + c2 * key2
            part_new_ref[2, h] = dif
            continue
        share = col(4)
        for a, x in ((0, out * share), (1, dif * (share * plan.scale))):
            if not isinstance(offset, int):
                x = pltpu.roll(x, (count - offset) % count, 0)
            of = slice(h * plan.head_size, (h + 1) * plan.head_size)
            if own_ref is not None:
                own_ref[a, :, of] = x[: plan.part_rows].astype(BF16)
                send_ref[a, :, of] = x[plan.part_rows : plan.last_rows].astype(BF16)
            else:
                send_ref[a, :, of] = x[: plan.last_rows].astype(BF16)
    if not last:
        after = plan.counts[k + 2]
        gone = pl.ds(aligned(plan.give(k + 1), after), after)
        for a in range(3):
            for h in range(plan.heads):
                send_ref[a, h] = part_new_ref[a, h, gone, :].astype(BF16)


def turn_body(pair_ref, turned_ref):
    for p in range(pair_ref.shape[0]):
        turned_ref[p] = pair_ref[p].T


def backward_body(plan, stat_ref, stat_all_ref, qb_ref, gb_ref, turned_ref, dk_ref, dv_ref, table, wk, wv):
    lanes = plan.lanes

    @pl.when(pl.program_id(0) == 0)
    def _():
        inverse = 1.0 / jnp.where(stat_all_ref[8:16] > 0.0, stat_all_ref[8:16], 1.0)
        f = jnp.exp(stat_ref[0:8] - stat_all_ref[0:8]) * inverse
        c = f * (stat_ref[16:24] - stat_all_ref[16:24])
        rest = jnp.zeros((128 - 24, lanes), F32)
        table[...] = jnp.concatenate([f, f * plan.scale, c * plan.scale, rest], axis=0).T
        for p in range(plan.groups):
            queries = qb_ref[p].astype(F32)
            wv[p] = (gb_ref[p].astype(F32) * table[:, p : p + 1]).astype(BF16)
            wk[p, :lanes] = (queries * table[:, 16 + p : 17 + p]).astype(BF16)
            wk[p, lanes:] = (queries * table[:, 8 + p : 9 + p]).astype(BF16)

    p = pl.program_id(0)
    dk_ref[...] = nn(turned_ref[0], wk[p]).astype(BF16)
    dv_ref[...] = nn(turned_ref[0, :, :lanes], wv[p]).astype(BF16)


def local(query_states, key_states, value_states, level_ids, level_bias, live_counts, out_grad):
    plan = Plan(query_states, key_states, level_bias)
    qi = lax.axis_index("query")
    size, slots, lanes, groups, heads = plan.head_size, plan.slots, plan.lanes, plan.groups, plan.heads
    width = plan.group * size
    pairwise = plan.query_ways == 2
    both = jnp.stack([query_states, out_grad])
    if pairwise:
        theirs = lax.dynamic_slice_in_dim(both, (1 - qi) * plan.features, plan.features, 2)
        moved = lax.ppermute(theirs, "query", [(0, 1), (1, 0)])
        row_inputs = (query_states, out_grad, moved)
    else:
        row_inputs = (lax.all_to_all(both, "query", split_axis=2, concat_axis=1, tiled=True),)
    table = lax.dynamic_slice_in_dim(level_bias, qi * heads, heads, 1)
    term = jnp.zeros((heads, slots), F32)
    for level in range(level_bias.shape[0]):
        term = jnp.where(level_ids[None, :] == level, table[level][:, None], term)
    slot = lax.broadcasted_iota(jnp.int32, (1, slots), 1)
    term = jnp.where(slot < live_counts[0], term, -1e30)

    stat_shape = jax.ShapeDtypeStruct((24, lanes), F32)
    block_shape = jax.ShapeDtypeStruct((groups, lanes, width), BF16)
    part_shape = lambda k: jax.ShapeDtypeStruct((3, heads, plan.counts[k], size), F32)
    send_shape = lambda k: jax.ShapeDtypeStruct((3, heads, plan.counts[k + 1], size), BF16)
    part, send, stat_own, pair, qb, gb = call(
        functools.partial(forward_body, plan, pairwise),
        (
            part_shape(0),
            send_shape(0),
            stat_shape,
            jax.ShapeDtypeStruct((groups, 2 * lanes, slots), BF16),
            block_shape,
            block_shape,
        ),
        24,
        4 * 10**9,
        in_specs=[VMEM] * (len(row_inputs) + 3),
        out_specs=[VMEM] * 6,
        scratch_shapes=[
            pltpu.VMEM((plan.rows, plan.features), BF16),
            pltpu.VMEM((lanes, slots), F32),
            pltpu.VMEM((lanes, slots), F32),
            pltpu.VMEM((lanes, 128), F32),
        ],
        name="forward",
    )(*row_inputs, key_states, value_states, term)

    turned = call(
        turn_body,
        jax.ShapeDtypeStruct((groups, slots, 2 * lanes), BF16),
        8,
        10**9,
        in_specs=[VMEM],
        out_specs=VMEM,
        name="turn",
    )(pair)

    stat = stat_own
    for k in range(plan.rounds):
        swap = [(i, i ^ (1 << k)) for i in range(plan.owner_ways)]
        came = lax.ppermute(send, "ctx", swap)
        stat_came = lax.ppermute(stat, "ctx", swap)
        last = k == plan.rounds - 1
        if not last:
            outs = (part_shape(k + 1), send_shape(k + 1), stat_shape)
        elif pairwise:
            rows_shape = jax.ShapeDtypeStruct((2, plan.part_rows, plan.features), BF16)
            outs = (stat_shape, rows_shape, rows_shape)
        else:
            outs = (stat_shape, jax.ShapeDtypeStruct((2, plan.last_rows, plan.features), BF16))
        body = functools.partial(merge_body, plan, k)
        if last and not pairwise:
            body = lambda a, b, c, d, s, o, t: merge_body(plan, plan.rounds - 1, a, b, c, d, s, None, o, t)
        result = call(
            body,
            outs,
            8,
            10**8,
            in_specs=[VMEM] * 4,
            out_specs=[VMEM] * len(outs),
            scratch_shapes=[pltpu.VMEM((lanes, 128), F32)],
            name=f"merge{k}",
        )(part, came, stat, stat_came)
        if not last:
            part, send, stat = result
    stat = result[0]
    if pairwise:
        own, away = result[1:]
        back = lax.ppermute(away, "query", [(0, 1), (1, 0)])

    key_grad, value_grad = call(
        functools.partial(backward_body, plan),
        (jax.ShapeDtypeStruct(key_states.shape, BF16), jax.ShapeDtypeStruct(value_states.shape, BF16)),
        16,
        4 * 10**9,
        grid=(groups,),
        in_specs=[
            pl.BlockSpec((24, lanes), lambda p: (0, 0)),
            pl.BlockSpec((24, lanes), lambda p: (0, 0)),
            pl.BlockSpec((groups, lanes, width), lambda p: (0, 0, 0)),
            pl.BlockSpec((groups, lanes, width), lambda p: (0, 0, 0)),
            pl.BlockSpec((1, slots, 2 * lanes), lambda p: (p, 0, 0)),
        ],
        out_specs=[pl.BlockSpec((slots, width), lambda p: (0, p))] * 2,
        scratch_shapes=[
            pltpu.VMEM((lanes, 128), F32),
            pltpu.VMEM((groups, 2 * lanes, width), BF16),
            pltpu.VMEM((groups, lanes, width), BF16),
        ],
        name="backward",
    )(stat_own, stat, qb, gb, turned)

    if pairwise:
        first = jnp.where(qi == 0, own, back)
        second = jnp.where(qi == 0, back, own)
        final = jnp.concatenate([first, second], axis=2)
    else:
        final = lax.all_to_all(result[1], "query", split_axis=1, concat_axis=2, tiled=True)
    return final[0], final[1], key_grad, value_grad


def solution(mesh):
    placed = (
        P("query", None),
        P("ctx", "query"),
        P("ctx", "query"),
        P("ctx"),
        P(),
        P("ctx"),
        P("query", None),
    )
    return jax.shard_map(
        local,
        mesh=mesh,
        in_specs=placed,
        out_specs=(
            P(("query", "ctx"), None),
            P(("query", "ctx"), None),
            P("ctx", "query"),
            P("ctx", "query"),
        ),
        check_vma=False,
    )
```

```python
import functools
import math

import jax
import jax.numpy as jnp
from jax import lax
from jax.experimental import pallas as pl
from jax.experimental.pallas import tpu as pltpu
from jax.sharding import PartitionSpec as P


F32 = jnp.float32
BF16 = jnp.bfloat16
MIB = 1024 * 1024
VMEM = pl.BlockSpec(memory_space=pltpu.VMEM)
HBM = pl.BlockSpec(memory_space=pltpu.HBM)


def call(body, out_shape, vmem_mib, flops, **kwargs):
    return pl.pallas_call(
        body,
        out_shape=out_shape,
        compiler_params=pltpu.CompilerParams(vmem_limit_bytes=vmem_mib * MIB),
        cost_estimate=pl.CostEstimate(flops=flops, bytes_accessed=MIB, transcendentals=0),
        **kwargs,
    )


def nt(a, b):
    return lax.dot_general(a, b, (((1,), (1,)), ((), ())), preferred_element_type=F32)


def nn(a, b):
    return lax.dot_general(a, b, (((1,), (0,)), ((), ())), preferred_element_type=F32)


class Plan:
    def __init__(self, query_states, key_states, level_bias):
        self.query_ways = lax.axis_size("query")
        self.owner_ways = lax.axis_size("ctx")
        self.slots, self.features = key_states.shape
        self.heads = level_bias.shape[1] // self.query_ways
        self.head_size = self.features // self.heads
        self.scale = 1.0 / math.sqrt(self.head_size)
        self.own_rows = query_states.shape[0]
        self.rows = self.own_rows * self.query_ways
        self.part_rows = self.own_rows // self.owner_ways
        self.last_rows = self.part_rows * self.query_ways
        self.group = 2 if self.heads % 2 == 0 and self.rows <= 128 else 1
        self.groups = self.heads // self.group
        self.lanes = self.group * self.rows
        self.rounds = self.owner_ways.bit_length() - 1
        assert 1 << self.rounds == self.owner_ways and self.groups <= 8
        counts = [self.rows]
        for _ in range(self.rounds):
            half = counts[-1] // 2
            counts.append(half if half >= 8 else counts[-1])
        self.counts = counts
        self.packed = None
        if self.rounds and counts[-2] == counts[-1] == 8 and self.rows >> self.rounds == 4 and self.group == 2:
            self.packed = self.rounds - 1

    def split(self, k):
        return k < self.rounds and self.counts[k + 1] < self.counts[k]

    def sent_heads(self, k):
        return self.heads // 2 if k == self.packed else self.heads

    def bit(self, k):
        return (lax.axis_index("ctx") >> k) & 1

    def keep(self, k):
        return self.bit(k) * self.counts[k + 1] if self.split(k) else 0

    def give(self, k):
        return (1 - self.bit(k)) * self.counts[k + 1] if self.split(k) else 0

    def base(self, k):
        return sum((self.keep(j) for j in range(k)), 0)

    def last_offset(self):
        offset = 0
        for k in range(self.rounds):
            if not self.split(k) and k != self.packed:
                offset = offset + self.bit(k) * (self.rows >> (k + 1))
        return offset


def aligned(x, by):
    return pl.multiple_of(x, by) if by >= 8 and not isinstance(x, int) else x


def halves(first, second, upper):
    top = lax.broadcasted_iota(jnp.int32, first.shape, 0) < 4
    lower_rows = jnp.where(top, first, pltpu.roll(second, 4, 0))
    upper_rows = jnp.where(top, pltpu.roll(first, 4, 0), second)
    return jnp.where(upper == 1, upper_rows, lower_rows)


def load_body(plan, split_parts, *refs):
    count = 4 if split_parts else 2
    ins, outs, semaphores = refs[:count], refs[count : 2 * count], refs[2 * count]
    copies = []
    for n, (source, target) in enumerate(zip(ins, outs)):
        if n >= 2:
            start = pl.multiple_of(lax.axis_index("query") * plan.features, 128)
            source = source.at[:, pl.ds(start, plan.features)]
        copies.append(pltpu.make_async_copy(source, target, semaphores.at[n]))
    for copy in copies:
        copy.start()
    for copy in copies:
        copy.wait()


def forward_body(plan, split_parts, *refs):
    if split_parts:
        q_ref, g_ref, moved_ref = refs[:3]
        refs = refs[3:]
    else:
        moved_ref = refs[0]
        refs = refs[1:]
    (k_ref, v_ref, term_ref, part_ref, send_ref, stat_ref, pair_ref, qb_ref, gb_ref) = refs[:9]
    source, scores, dprobs, columns = refs[9:]
    rows, size, group = plan.rows, plan.head_size, plan.group
    width = group * size
    place = lax.broadcasted_iota(jnp.int32, (rows, rows), 0)
    column = lax.broadcasted_iota(jnp.int32, (rows, rows), 1)
    inner = place % plan.last_rows
    outer = place // plan.last_rows
    owner = jnp.zeros_like(outer)
    for k in range(plan.rounds):
        owner = owner | (((outer >> (plan.rounds - 1 - k)) & 1) << k)
    wanted = (
        inner // plan.part_rows * plan.own_rows + owner * plan.part_rows + inner % plan.part_rows
    )
    permute = (column == wanted).astype(F32).astype(BF16)
    qb_ref[...] = jnp.zeros_like(qb_ref)
    gb_ref[...] = jnp.zeros_like(gb_ref)
    for which, own_ref, block_ref in ((0, 0, qb_ref), (1, 1, gb_ref)):
        if split_parts:
            source[: plan.own_rows] = (q_ref, g_ref)[own_ref][...]
            source[plan.own_rows :] = moved_ref[which]
        else:
            source[...] = moved_ref[which]
        for p in range(plan.groups):
            ordered = nn(permute, source[:, p * width : (p + 1) * width]).astype(BF16)
            for q in range(group):
                block_ref[p, q * rows : (q + 1) * rows, q * size : (q + 1) * size] = ordered[
                    :, q * size : (q + 1) * size
                ]
    columns[...] = jnp.zeros_like(columns)
    step = 16
    for p in range(plan.groups):
        keys = k_ref[:, p * width : (p + 1) * width]
        values = v_ref[:, p * width : (p + 1) * width]
        scores[p % 2] = nt(qb_ref[p], keys)
        dprobs[p % 2] = nt(gb_ref[p], values)
        for r in range(0, plan.lanes, step):
            h = p * group + r // rows
            s = scores[p % 2, r : r + step] * plan.scale + term_ref[h : h + 1, :]
            top = jnp.max(s, axis=1, keepdims=True)
            e = jnp.exp(s - top)
            total = jnp.sum(e, axis=1, keepdims=True)
            d = dprobs[p % 2, r : r + step]
            mean = jnp.sum(e * d, axis=1, keepdims=True) / total
            pair_ref[p, r : r + step, :] = e.astype(BF16)
            pair_ref[p, plan.lanes + r : plan.lanes + r + step, :] = (e * (d - mean)).astype(BF16)
            columns[r : r + step, p : p + 1] = top
            columns[r : r + step, 8 + p : 9 + p] = total
            columns[r : r + step, 16 + p : 17 + p] = mean
        with_values = nn(pair_ref[p, : plan.lanes, :], values)
        with_keys = nn(pair_ref[p], keys)
        for q in range(group):
            at = slice(q * rows, (q + 1) * rows)
            of = slice(q * size, (q + 1) * size)
            part_ref[0, p * group + q] = with_values[at, of]
            part_ref[1, p * group + q] = with_keys[at, of]
            part_ref[2, p * group + q] = with_keys[plan.lanes + q * rows : plan.lanes + (q + 1) * rows, of]
    give(plan, 0, part_ref, send_ref)
    stat_ref[...] = columns[...].T[:24]


def statistics(stat_ref, stat_came_ref):
    top1, total1, mean1 = (stat_ref[8 * t : 8 * t + 8] for t in range(3))
    top2, total2, mean2 = (stat_came_ref[8 * t : 8 * t + 8] for t in range(3))
    top = jnp.maximum(top1, top2)
    f1 = jnp.exp(top1 - top)
    f2 = jnp.exp(top2 - top)
    total = f1 * total1 + f2 * total2
    inverse = 1.0 / jnp.where(total > 0.0, total, 1.0)
    w1 = f1 * total1 * inverse
    w2 = f2 * total2 * inverse
    gap = mean1 - mean2
    merged = (top, total, mean1 * w1 + mean2 * w2)
    return merged, (f1, f2, f1 * w2 * gap, -f2 * w1 * gap, inverse)


def merge_statistics_body(stat_ref, stat_came_ref, stat_new_ref):
    merged, _ = statistics(stat_ref, stat_came_ref)
    for t in range(3):
        stat_new_ref[8 * t : 8 * t + 8] = merged[t]


def merge_body(plan, k, part_ref, came_ref, stat_ref, stat_came_ref, *refs):
    last = k == plan.rounds - 1
    if last:
        own_ref, away_ref, table = refs if len(refs) == 3 else (None, *refs)
    else:
        part_new_ref, send_ref, table = refs
    _, factors = statistics(stat_ref, stat_came_ref)
    rest = jnp.zeros((128 - 40, plan.lanes), F32)
    table[...] = jnp.concatenate([*factors, rest], axis=0).T
    count = plan.counts[k + 1]
    kept = pl.ds(aligned(plan.keep(k), count), count)
    base = plan.base(k + 1)
    rows_of = [pl.ds(aligned(q * plan.rows + base, count), count) for q in range(plan.group)]
    packed = k == plan.packed
    bit = plan.bit(k)
    if packed:
        joined = halves(table[rows_of[0], :], table[rows_of[1], :], bit)
    for n in range(plan.sent_heads(k)):
        if packed:
            p = n
            mine = [halves(part_ref[a, 2 * n], part_ref[a, 2 * n + 1], bit) for a in range(3)]
            rows = joined
        else:
            p = n // plan.group
            mine = [part_ref[a, n, kept, :] for a in range(3)]
            rows = table[rows_of[n % plan.group], :]
        col = lambda t: rows[:, 8 * t + p : 8 * t + p + 1]
        out1, key1, dif1 = mine
        out2, key2, dif2 = (came_ref[a, n].astype(F32) for a in range(3))
        c1, c2 = col(0), col(1)
        out = c1 * out1 + c2 * out2
        dif = c1 * dif1 + c2 * dif2 + col(2) * key1 + col(3) * key2
        if not last:
            part_new_ref[0, n] = out
            part_new_ref[1, n] = c1 * key1 + c2 * key2
            part_new_ref[2, n] = dif
            continue
        share = col(4)
        for a, x in ((0, out * share), (1, dif * (share * plan.scale))):
            offset = plan.last_offset()
            if not isinstance(offset, int):
                x = pltpu.roll(x, (count - offset) % count, 0)
            for h, start in ((2 * n, 0), (2 * n + 1, 4)) if packed else ((n, 0),):
                of = slice(h * plan.head_size, (h + 1) * plan.head_size)
                middle, end = start + plan.part_rows, start + plan.last_rows
                if own_ref is not None:
                    own_ref[a, :, of] = x[start:middle].astype(BF16)
                    away_ref[a, :, of] = x[middle:end].astype(BF16)
                else:
                    away_ref[a, :, of] = x[start:end].astype(BF16)
    if not last:
        give(plan, k + 1, part_new_ref, send_ref)


def give(plan, k, part_ref, send_ref):
    if k == plan.packed:
        for a in range(3):
            for n in range(plan.heads // 2):
                x = halves(part_ref[a, 2 * n], part_ref[a, 2 * n + 1], 1 - plan.bit(k))
                send_ref[a, n] = x.astype(BF16)
        return
    count = plan.counts[k + 1]
    gone = pl.ds(aligned(plan.give(k), count), count)
    for a in range(3):
        for h in range(plan.heads):
            send_ref[a, h] = part_ref[a, h, gone, :].astype(BF16)


def turn_body(pair_ref, turned_ref):
    for p in range(pair_ref.shape[0]):
        turned_ref[p] = pair_ref[p].T


def backward_body(plan, stat_ref, stat_all_ref, qb_ref, gb_ref, turned_ref, dk_ref, dv_ref, table, dk, dv, semaphores):
    lanes = plan.lanes
    width = dk.shape[2]
    total = stat_all_ref[8:16]
    inverse = 1.0 / jnp.where(total > 0.0, total, 1.0)
    f = jnp.exp(stat_ref[0:8] - stat_all_ref[0:8]) * inverse
    c = f * (stat_ref[16:24] - stat_all_ref[16:24])
    rest = jnp.zeros((128 - 24, lanes), F32)
    table[...] = jnp.concatenate([f, f * plan.scale, c * plan.scale, rest], axis=0).T
    copies = []
    for p in range(plan.groups):
        queries = qb_ref[p].astype(F32)
        wv = (gb_ref[p].astype(F32) * table[:, p : p + 1]).astype(BF16)
        wc = (queries * table[:, 16 + p : 17 + p]).astype(BF16)
        wf = (queries * table[:, 8 + p : 9 + p]).astype(BF16)
        for n, (buffer, target) in enumerate(((dk, dk_ref), (dv, dv_ref))):
            if n == 0:
                buffer[p] = nn(turned_ref[p], jnp.concatenate([wc, wf], axis=0)).astype(BF16)
            else:
                buffer[p] = nn(turned_ref[p, :, :lanes], wv).astype(BF16)
            copy = pltpu.make_async_copy(
                buffer.at[p], target.at[:, p * width : (p + 1) * width], semaphores.at[n, p]
            )
            copy.start()
            copies.append(copy)
    for copy in copies:
        copy.wait()


def local(query_states, key_states, value_states, level_ids, level_bias, live_counts, out_grad):
    plan = Plan(query_states, key_states, level_bias)
    qi = lax.axis_index("query")
    size, slots, lanes, groups, heads = plan.head_size, plan.slots, plan.lanes, plan.groups, plan.heads
    width = plan.group * size
    pairwise = plan.query_ways == 2
    both = jnp.stack([query_states, out_grad])
    if pairwise:
        theirs = lax.dynamic_slice_in_dim(both, (1 - qi) * plan.features, plan.features, 2)
        moved = lax.ppermute(theirs, "query", [(0, 1), (1, 0)])
    else:
        moved = lax.all_to_all(both, "query", split_axis=2, concat_axis=1, tiled=True)
    table = lax.dynamic_slice_in_dim(level_bias, qi * heads, heads, 1)
    term = jnp.zeros((heads, slots), F32)
    for level in range(level_bias.shape[0]):
        term = jnp.where(level_ids[None, :] == level, table[level][:, None], term)
    slot = lax.broadcasted_iota(jnp.int32, (1, slots), 1)
    term = jnp.where(slot < live_counts[0], term, -1e30)

    stat_shape = jax.ShapeDtypeStruct((24, lanes), F32)
    block_shape = jax.ShapeDtypeStruct((groups, lanes, width), BF16)
    part_shape = lambda k: jax.ShapeDtypeStruct((3, heads, plan.counts[k], size), F32)
    send_shape = lambda k: jax.ShapeDtypeStruct(
        (3, plan.sent_heads(k), plan.counts[k + 1], size), BF16
    )
    from_hbm = [key_states, value_states] + ([query_states, out_grad] if pairwise else [])
    from_hbm = [pltpu.with_memory_space_constraint(x, pltpu.HBM) for x in from_hbm]
    own_shape = jax.ShapeDtypeStruct((plan.own_rows, plan.features), BF16)
    context_shape = jax.ShapeDtypeStruct(key_states.shape, BF16)
    keys, values, *own_rows = call(
        functools.partial(load_body, plan, pairwise),
        [context_shape] * 2 + [own_shape] * (len(from_hbm) - 2),
        2,
        10**9,
        in_specs=[HBM] * len(from_hbm),
        out_specs=[VMEM] * len(from_hbm),
        scratch_shapes=[pltpu.SemaphoreType.DMA((len(from_hbm),))],
        name="load",
    )(*from_hbm)
    part, send, stat_own, pair, qb, gb = call(
        functools.partial(forward_body, plan, pairwise),
        (
            part_shape(0),
            send_shape(0),
            stat_shape,
            jax.ShapeDtypeStruct((groups, 2 * lanes, slots), BF16),
            block_shape,
            block_shape,
        ),
        12,
        4 * 10**9,
        in_specs=[VMEM] * (len(own_rows) + 4),
        out_specs=[VMEM] * 6,
        scratch_shapes=[
            pltpu.VMEM((plan.rows, plan.features), BF16),
            pltpu.VMEM((2, lanes, slots), F32),
            pltpu.VMEM((2, lanes, slots), F32),
            pltpu.VMEM((lanes, 128), F32),
        ],
        name="forward",
    )(*own_rows, moved, keys, values, term)

    turned = call(
        turn_body,
        jax.ShapeDtypeStruct((groups, slots, 2 * lanes), BF16),
        4,
        10**9,
        in_specs=[VMEM],
        out_specs=VMEM,
        name="turn",
    )(pair)

    stat = stat_own
    for k in range(plan.rounds):
        swap = [(i, i ^ (1 << k)) for i in range(plan.owner_ways)]
        stat_came = lax.ppermute(stat, "ctx", swap)
        came = lax.ppermute(send, "ctx", swap)
        merged = call(
            merge_statistics_body,
            stat_shape,
            2,
            10**6,
            in_specs=[VMEM] * 2,
            out_specs=VMEM,
            name=f"statistics{k}",
        )(stat, stat_came)
        if k < plan.rounds - 1:
            outs = (part_shape(k + 1), send_shape(k + 1))
        elif pairwise:
            outs = (jax.ShapeDtypeStruct((2, plan.part_rows, plan.features), BF16),) * 2
        else:
            outs = (jax.ShapeDtypeStruct((2, plan.last_rows, plan.features), BF16),)
        part, send, *_ = call(
            functools.partial(merge_body, plan, k),
            outs,
            4,
            10**8,
            in_specs=[VMEM] * 4,
            out_specs=[VMEM] * len(outs),
            scratch_shapes=[pltpu.VMEM((lanes, 128), F32)],
            name=f"merge{k}",
        )(part, came, stat, stat_came) + (None,) * (2 - len(outs))
        stat = merged
    if pairwise:
        own, away = part, send
        back = lax.ppermute(away, "query", [(0, 1), (1, 0)])

    key_grad, value_grad = call(
        functools.partial(backward_body, plan),
        (context_shape, context_shape),
        12,
        4 * 10**9,
        in_specs=[VMEM] * 5,
        out_specs=[HBM] * 2,
        scratch_shapes=[
            pltpu.VMEM((lanes, 128), F32),
            pltpu.VMEM((groups, slots, width), BF16),
            pltpu.VMEM((groups, slots, width), BF16),
            pltpu.SemaphoreType.DMA((2, groups)),
        ],
        name="backward",
    )(stat_own, stat, qb, gb, turned)

    if pairwise:
        first = jnp.where(qi == 0, own, back)
        second = jnp.where(qi == 0, back, own)
        final = jnp.concatenate([first, second], axis=2)
    else:
        final = lax.all_to_all(part, "query", split_axis=1, concat_axis=2, tiled=True)
    return final[0], final[1], key_grad, value_grad


def solution(mesh):
    placed = (
        P("query", None),
        P("ctx", "query"),
        P("ctx", "query"),
        P("ctx"),
        P(),
        P("ctx"),
        P("query", None),
    )

    return jax.shard_map(
        local,
        mesh=mesh,
        in_specs=placed,
        out_specs=(
            P(("query", "ctx"), None),
            P(("query", "ctx"), None),
            P("ctx", "query"),
            P("ctx", "query"),
        ),
        check_vma=False,
    )
```

```python
import functools
import math

import jax
import jax.numpy as jnp
from jax import lax
from jax.experimental import pallas as pl
from jax.experimental.pallas import tpu as pltpu
from jax.sharding import PartitionSpec as P


F32 = jnp.float32
BF16 = jnp.bfloat16
MIB = 1024 * 1024
VMEM = pl.BlockSpec(memory_space=pltpu.VMEM)
HBM = pl.BlockSpec(memory_space=pltpu.HBM)


def call(body, out_shape, vmem_mib, flops, **kwargs):
    return pl.pallas_call(
        body,
        out_shape=out_shape,
        compiler_params=pltpu.CompilerParams(vmem_limit_bytes=vmem_mib * MIB),
        cost_estimate=pl.CostEstimate(flops=flops, bytes_accessed=MIB, transcendentals=0),
        **kwargs,
    )


def nt(a, b):
    return lax.dot_general(a, b, (((1,), (1,)), ((), ())), preferred_element_type=F32)


def nn(a, b):
    return lax.dot_general(a, b, (((1,), (0,)), ((), ())), preferred_element_type=F32)


class Plan:
    def __init__(self, query_states, key_states, level_bias):
        self.query_ways = lax.axis_size("query")
        self.owner_ways = lax.axis_size("ctx")
        self.slots, self.features = key_states.shape
        self.heads = level_bias.shape[1] // self.query_ways
        self.head_size = self.features // self.heads
        self.scale = 1.0 / math.sqrt(self.head_size)
        self.own_rows = query_states.shape[0]
        self.rows = self.own_rows * self.query_ways
        self.part_rows = self.own_rows // self.owner_ways
        self.last_rows = self.part_rows * self.query_ways
        self.group = 2 if self.heads % 2 == 0 and self.rows <= 128 else 1
        self.groups = self.heads // self.group
        self.lanes = self.group * self.rows
        self.rounds = self.owner_ways.bit_length() - 1
        assert 1 << self.rounds == self.owner_ways and self.groups <= 8
        counts = [self.rows]
        for _ in range(self.rounds):
            half = counts[-1] // 2
            counts.append(half if half >= 8 else counts[-1])
        self.counts = counts
        self.direct = self.query_ways == 2 and self.rounds >= 3 and counts[-2] == 2 * self.last_rows >= 8

    def split(self, k):
        return k < self.rounds and self.counts[k + 1] < self.counts[k]

    def bit(self, k):
        return (lax.axis_index("ctx") >> k) & 1

    def keep(self, k):
        return self.bit(k) * self.counts[k + 1] if self.split(k) else 0

    def give(self, k):
        return (1 - self.bit(k)) * self.counts[k + 1] if self.split(k) else 0

    def base(self, k):
        return sum((self.keep(j) for j in range(k)), 0)

    def last_offset(self):
        offset = 0
        for k in range(self.rounds):
            if not self.split(k):
                offset = offset + self.bit(k) * (self.rows >> (k + 1))
        return offset


def aligned(x, by):
    return pl.multiple_of(x, by) if by >= 8 and not isinstance(x, int) else x


def load_body(plan, split_parts, *refs):
    count = 4 if split_parts else 2
    ins, outs, semaphores = refs[:count], refs[count : 2 * count], refs[2 * count]
    copies = []
    for n, (source, target) in enumerate(zip(ins, outs)):
        if n >= 2:
            start = pl.multiple_of(lax.axis_index("query") * plan.features, 128)
            source = source.at[:, pl.ds(start, plan.features)]
        copies.append(pltpu.make_async_copy(source, target, semaphores.at[n]))
    for copy in copies:
        copy.start()
    for copy in copies:
        copy.wait()


def forward_body(plan, split_parts, *refs):
    if split_parts:
        q_ref, g_ref, moved_ref = refs[:3]
        refs = refs[3:]
    else:
        moved_ref = refs[0]
        refs = refs[1:]
    (k_ref, v_ref, term_ref, part_ref, send_ref, stat_ref, pair_ref, qb_ref, gb_ref) = refs[:9]
    source, scores, dprobs, columns = refs[9:]
    rows, size, group = plan.rows, plan.head_size, plan.group
    width = group * size
    place = lax.broadcasted_iota(jnp.int32, (rows, rows), 0)
    column = lax.broadcasted_iota(jnp.int32, (rows, rows), 1)
    inner = place % plan.last_rows
    outer = place // plan.last_rows
    owner = jnp.zeros_like(outer)
    for k in range(plan.rounds):
        owner = owner | (((outer >> (plan.rounds - 1 - k)) & 1) << k)
    wanted = (
        inner // plan.part_rows * plan.own_rows + owner * plan.part_rows + inner % plan.part_rows
    )
    permute = (column == wanted).astype(F32).astype(BF16)
    qb_ref[...] = jnp.zeros_like(qb_ref)
    gb_ref[...] = jnp.zeros_like(gb_ref)
    for which, own_ref, block_ref in ((0, 0, qb_ref), (1, 1, gb_ref)):
        if split_parts:
            source[: plan.own_rows] = (q_ref, g_ref)[own_ref][...]
            source[plan.own_rows :] = moved_ref[which]
        else:
            source[...] = moved_ref[which]
        for p in range(plan.groups):
            ordered = nn(permute, source[:, p * width : (p + 1) * width]).astype(BF16)
            for q in range(group):
                block_ref[p, q * rows : (q + 1) * rows, q * size : (q + 1) * size] = ordered[
                    :, q * size : (q + 1) * size
                ]
    columns[...] = jnp.zeros_like(columns)
    step = 16
    for p in range(plan.groups):
        keys = k_ref[:, p * width : (p + 1) * width]
        values = v_ref[:, p * width : (p + 1) * width]
        scores[p % 2] = nt(qb_ref[p], keys)
        dprobs[p % 2] = nt(gb_ref[p], values)
        for r in range(0, plan.lanes, step):
            h = p * group + r // rows
            s = scores[p % 2, r : r + step] * plan.scale + term_ref[h : h + 1, :]
            top = jnp.max(s, axis=1, keepdims=True)
            e = jnp.exp(s - top)
            total = jnp.sum(e, axis=1, keepdims=True)
            d = dprobs[p % 2, r : r + step]
            mean = jnp.sum(e * d, axis=1, keepdims=True) / total
            pair_ref[p, r : r + step, :] = e.astype(BF16)
            pair_ref[p, plan.lanes + r : plan.lanes + r + step, :] = (e * (d - mean)).astype(BF16)
            columns[r : r + step, p : p + 1] = top
            columns[r : r + step, 8 + p : 9 + p] = total
            columns[r : r + step, 16 + p : 17 + p] = mean
        with_values = nn(pair_ref[p, : plan.lanes, :], values)
        with_keys = nn(pair_ref[p], keys)
        for q in range(group):
            at = slice(q * rows, (q + 1) * rows)
            of = slice(q * size, (q + 1) * size)
            part_ref[0, p * group + q] = with_values[at, of]
            part_ref[1, p * group + q] = with_keys[at, of]
            part_ref[2, p * group + q] = with_keys[plan.lanes + q * rows : plan.lanes + (q + 1) * rows, of]
    give(plan, 0, part_ref, send_ref)
    stat_ref[...] = columns[...].T[:24]


def statistics(stat_ref, stat_came_ref):
    top1, total1, mean1 = (stat_ref[8 * t : 8 * t + 8] for t in range(3))
    top2, total2, mean2 = (stat_came_ref[8 * t : 8 * t + 8] for t in range(3))
    top = jnp.maximum(top1, top2)
    f1 = jnp.exp(top1 - top)
    f2 = jnp.exp(top2 - top)
    total = f1 * total1 + f2 * total2
    inverse = 1.0 / jnp.where(total > 0.0, total, 1.0)
    w1 = f1 * total1 * inverse
    w2 = f2 * total2 * inverse
    gap = mean1 - mean2
    merged = (top, total, mean1 * w1 + mean2 * w2)
    return merged, (f1, f2, f1 * w2 * gap, -f2 * w1 * gap, inverse)


def merge_statistics_body(stat_ref, stat_came_ref, stat_new_ref):
    merged, _ = statistics(stat_ref, stat_came_ref)
    for t in range(3):
        stat_new_ref[8 * t : 8 * t + 8] = merged[t]


def merge_body(plan, k, part_ref, came_ref, stat_ref, stat_came_ref, *refs):
    last = k == plan.rounds - 1
    if last:
        rows_ref, table = refs
    else:
        part_new_ref, send_ref, table = refs
    _, factors = statistics(stat_ref, stat_came_ref)
    rest = jnp.zeros((128 - 40, plan.lanes), F32)
    table[...] = jnp.concatenate([*factors, rest], axis=0).T
    count = plan.counts[k + 1]
    kept = pl.ds(aligned(plan.keep(k), count), count)
    base = plan.base(k + 1)
    rows_of = [pl.ds(aligned(q * plan.rows + base, count), count) for q in range(plan.group)]
    for h in range(plan.heads):
        p = h // plan.group
        rows = table[rows_of[h % plan.group], :]
        col = lambda t: rows[:, 8 * t + p : 8 * t + p + 1]
        out1, key1, dif1 = (part_ref[a, h, kept, :] for a in range(3))
        out2, key2, dif2 = (came_ref[a, h].astype(F32) for a in range(3))
        c1, c2 = col(0), col(1)
        out = c1 * out1 + c2 * out2
        dif = c1 * dif1 + c2 * dif2 + col(2) * key1 + col(3) * key2
        if not last:
            part_new_ref[0, h] = out
            part_new_ref[1, h] = c1 * key1 + c2 * key2
            part_new_ref[2, h] = dif
            continue
        share = col(4)
        for a, x in ((0, out * share), (1, dif * (share * plan.scale))):
            offset = plan.last_offset()
            if not isinstance(offset, int):
                x = pltpu.roll(x, (count - offset) % count, 0)
            of = slice(h * plan.head_size, (h + 1) * plan.head_size)
            rows_ref[a, :, of] = x[: plan.last_rows].astype(BF16)
    if not last:
        give(plan, k + 1, part_new_ref, send_ref)


def finish_body(plan, part_ref, came_ref, stat_ref, stat_came_ref, stat_all_ref, own_ref, *refs):
    *away_refs, table = refs
    k = plan.rounds - 2
    top, total, mean = (stat_all_ref[8 * t : 8 * t + 8] for t in range(3))
    inverse = 1.0 / jnp.where(total > 0.0, total, 1.0)
    factors = []
    for ref in (stat_ref, stat_came_ref):
        f = jnp.exp(ref[0:8] - top) * inverse
        factors += [f, f * plan.scale, f * plan.scale * (ref[16:24] - mean)]
    rest = jnp.zeros((128 - 48, plan.lanes), F32)
    table[...] = jnp.concatenate([*factors, rest], axis=0).T
    count = plan.counts[k + 1]
    kept = pl.ds(aligned(plan.keep(k), count), count)
    base = plan.base(k + 1)
    rows_of = [pl.ds(aligned(q * plan.rows + base, count), count) for q in range(plan.group)]
    turn = plan.bit(k + 1) * plan.last_rows
    for h in range(plan.heads):
        p = h // plan.group
        rows = table[rows_of[h % plan.group], :]
        col = lambda t: rows[:, 8 * t + p : 8 * t + p + 1]
        out1, key1, dif1 = (part_ref[a, h, kept, :] for a in range(3))
        out2, key2, dif2 = (came_ref[a, h].astype(F32) for a in range(3))
        out = col(0) * out1 + col(3) * out2
        dif = col(1) * dif1 + col(4) * dif2 + col(2) * key1 + col(5) * key2
        of = slice(h * plan.head_size, (h + 1) * plan.head_size)
        for a, x in ((0, out), (1, dif)):
            x = pltpu.roll(x, (count - turn) % count, 0)
            for n, ref in enumerate((own_ref, *away_refs)):
                ref[a, :, of] = x[n * plan.part_rows : (n + 1) * plan.part_rows].astype(ref.dtype)


def gather_body(plan, own_ref, query_ref, owner_ref, both_ref, attn_ref, dq_ref):
    me = lax.axis_index("query")
    for a, out_ref in ((0, attn_ref), (1, dq_ref)):
        mine = own_ref[a] + owner_ref[a].astype(F32)
        theirs = query_ref[a].astype(F32) + both_ref[a].astype(F32)
        for at, x in ((me, mine), (1 - me, theirs)):
            start = pl.multiple_of(at * plan.features, 128)
            out_ref[:, pl.ds(start, plan.features)] = x.astype(BF16)


def give(plan, k, part_ref, send_ref):
    count = plan.counts[k + 1]
    gone = pl.ds(aligned(plan.give(k), count), count)
    for a in range(3):
        for h in range(plan.heads):
            send_ref[a, h] = part_ref[a, h, gone, :].astype(BF16)


def turn_body(pair_ref, turned_ref):
    for p in range(pair_ref.shape[0]):
        turned_ref[p] = pair_ref[p].T


def backward_body(plan, first, count, stat_ref, stat_all_ref, qb_ref, gb_ref, turned_ref, *refs):
    dk_ref, dv_ref, table, dk, dv, semaphores = refs[-6:]
    lanes = plan.lanes
    width = dk.shape[2]
    total = stat_all_ref[8:16]
    inverse = 1.0 / jnp.where(total > 0.0, total, 1.0)
    f = jnp.exp(stat_ref[0:8] - stat_all_ref[0:8]) * inverse
    c = f * (stat_ref[16:24] - stat_all_ref[16:24])
    rest = jnp.zeros((128 - 24, lanes), F32)
    table[...] = jnp.concatenate([f, f * plan.scale, c * plan.scale, rest], axis=0).T
    copies = []
    for p in range(first, first + count):
        queries = qb_ref[p].astype(F32)
        wv = (gb_ref[p].astype(F32) * table[:, p : p + 1]).astype(BF16)
        wc = (queries * table[:, 16 + p : 17 + p]).astype(BF16)
        wf = (queries * table[:, 8 + p : 9 + p]).astype(BF16)
        for n, (buffer, target) in enumerate(((dk, dk_ref), (dv, dv_ref))):
            if n == 0:
                buffer[p - first] = nn(turned_ref[p], jnp.concatenate([wc, wf], axis=0)).astype(BF16)
            else:
                buffer[p - first] = nn(turned_ref[p, :, :lanes], wv).astype(BF16)
            copy = pltpu.make_async_copy(
                buffer.at[p - first], target.at[:, p * width : (p + 1) * width], semaphores.at[n, p - first]
            )
            copy.start()
            copies.append(copy)
    for copy in copies:
        copy.wait()


def local(query_states, key_states, value_states, level_ids, level_bias, live_counts, out_grad):
    plan = Plan(query_states, key_states, level_bias)
    qi = lax.axis_index("query")
    size, slots, lanes, groups, heads = plan.head_size, plan.slots, plan.lanes, plan.groups, plan.heads
    width = plan.group * size
    pairwise = plan.query_ways == 2
    both = jnp.stack([query_states, out_grad])
    if pairwise:
        theirs = lax.dynamic_slice_in_dim(both, (1 - qi) * plan.features, plan.features, 2)
        moved = lax.ppermute(theirs, "query", [(0, 1), (1, 0)])
    else:
        moved = lax.all_to_all(both, "query", split_axis=2, concat_axis=1, tiled=True)
    table = lax.dynamic_slice_in_dim(level_bias, qi * heads, heads, 1)
    term = jnp.zeros((heads, slots), F32)
    for level in range(level_bias.shape[0]):
        term = jnp.where(level_ids[None, :] == level, table[level][:, None], term)
    slot = lax.broadcasted_iota(jnp.int32, (1, slots), 1)
    term = jnp.where(slot < live_counts[0], term, -1e30)

    stat_shape = jax.ShapeDtypeStruct((24, lanes), F32)
    block_shape = jax.ShapeDtypeStruct((groups, lanes, width), BF16)
    part_shape = lambda k: jax.ShapeDtypeStruct((3, heads, plan.counts[k], size), F32)
    send_shape = lambda k: jax.ShapeDtypeStruct((3, heads, plan.counts[k + 1], size), BF16)
    from_hbm = [key_states, value_states] + ([query_states, out_grad] if pairwise else [])
    from_hbm = [pltpu.with_memory_space_constraint(x, pltpu.HBM) for x in from_hbm]
    own_shape = jax.ShapeDtypeStruct((plan.own_rows, plan.features), BF16)
    context_shape = jax.ShapeDtypeStruct(key_states.shape, BF16)
    keys, values, *own_rows = call(
        functools.partial(load_body, plan, pairwise),
        [context_shape] * 2 + [own_shape] * (len(from_hbm) - 2),
        2,
        10**9,
        in_specs=[HBM] * len(from_hbm),
        out_specs=[VMEM] * len(from_hbm),
        scratch_shapes=[pltpu.SemaphoreType.DMA((len(from_hbm),))],
        name="load",
    )(*from_hbm)
    part, send, stat_own, pair, qb, gb = call(
        functools.partial(forward_body, plan, pairwise),
        (
            part_shape(0),
            send_shape(0),
            stat_shape,
            jax.ShapeDtypeStruct((groups, 2 * lanes, slots), BF16),
            block_shape,
            block_shape,
        ),
        12,
        4 * 10**9,
        in_specs=[VMEM] * (len(own_rows) + 4),
        out_specs=[VMEM] * 6,
        scratch_shapes=[
            pltpu.VMEM((plan.rows, plan.features), BF16),
            pltpu.VMEM((2, lanes, slots), F32),
            pltpu.VMEM((2, lanes, slots), F32),
            pltpu.VMEM((lanes, 128), F32),
        ],
        name="forward",
    )(*own_rows, moved, keys, values, term)

    turned = call(
        turn_body,
        jax.ShapeDtypeStruct((groups, slots, 2 * lanes), BF16),
        4,
        10**9,
        in_specs=[VMEM],
        out_specs=VMEM,
        name="turn",
    )(pair)

    def swap(k):
        return [(i, i ^ (1 << k)) for i in range(plan.owner_ways)]

    def kernel(name, body, outs, *ins, vmem_mib=4, flops=10**8):
        return call(
            body,
            outs,
            vmem_mib,
            flops,
            in_specs=[VMEM] * len(ins),
            out_specs=[VMEM] * len(outs),
            scratch_shapes=[pltpu.VMEM((lanes, 128), F32)],
            name=name,
        )(*ins)

    def exchange_statistics(k, stat):
        came = lax.ppermute(stat, "ctx", swap(k))
        merged = call(
            merge_statistics_body,
            stat_shape,
            2,
            10**6,
            in_specs=[VMEM] * 2,
            out_specs=VMEM,
            name=f"statistics{k}",
        )(stat, came)
        return came, merged

    stats = [stat_own]
    stats_came = []
    for k in range(plan.rounds):
        came, merged = exchange_statistics(k, stats[k])
        stats_came.append(came)
        stats.append(merged)
    stat_all = stats[-1]

    def gradients(name, first, count, *into):
        return call(
            functools.partial(backward_body, plan, first, count),
            (context_shape, context_shape),
            8,
            4 * 10**9,
            in_specs=[VMEM] * 5 + [HBM] * len(into),
            out_specs=[HBM] * 2,
            scratch_shapes=[
                pltpu.VMEM((lanes, 128), F32),
                pltpu.VMEM((count, slots, width), BF16),
                pltpu.VMEM((count, slots, width), BF16),
                pltpu.SemaphoreType.DMA((2, count)),
            ],
            input_output_aliases={5 + n: n for n in range(len(into))},
            name=name,
        )(stat_own, stat_all, qb, gb, turned, *into)

    split = (groups + 1) // 2
    grads = gradients("backward0", 0, split)
    grads = gradients("backward1", split, groups - split, *grads)

    for k in range(plan.rounds):
        if plan.direct and k == plan.rounds - 1:
            continue
        came = lax.ppermute(send, "ctx", swap(k))
        inputs = (part, came, stats[k], stats_came[k])
        if plan.direct and k == plan.rounds - 2:
            rows_shape = lambda dtype: jax.ShapeDtypeStruct((2, plan.part_rows, plan.features), dtype)
            own, *away = kernel(
                "finish",
                functools.partial(finish_body, plan),
                (rows_shape(F32),) + (rows_shape(BF16),) * 3,
                *inputs,
                stat_all,
            )
        elif k < plan.rounds - 1:
            part, send = kernel(
                f"merge{k}",
                functools.partial(merge_body, plan, k),
                (part_shape(k + 1), send_shape(k + 1)),
                *inputs,
            )
        else:
            (rows,) = kernel(
                f"merge{k}",
                functools.partial(merge_body, plan, k),
                (jax.ShapeDtypeStruct((2, plan.last_rows, plan.features), BF16),),
                *inputs,
            )
    if not plan.direct:
        final = lax.all_to_all(rows, "query", split_axis=1, concat_axis=2, tiled=True)
        return final[0], final[1], *grads

    ways = plan.owner_ways
    both_axes = ("query", "ctx")
    jump = ways >> 1
    from_query = lax.ppermute(away[0], "query", [(0, 1), (1, 0)])
    from_owner = lax.ppermute(away[1], "ctx", swap(plan.rounds - 1))
    from_both = lax.ppermute(away[2], both_axes, [(i, i ^ ways ^ jump) for i in range(2 * ways)])
    outs = (jax.ShapeDtypeStruct((plan.part_rows, 2 * plan.features), BF16),) * 2
    attn, query_grad = call(
        functools.partial(gather_body, plan),
        outs,
        2,
        10**6,
        in_specs=[VMEM] * 4,
        out_specs=[VMEM] * 2,
        name="gather",
    )(own, from_query, from_owner, from_both)
    return attn, query_grad, *grads


def solution(mesh):
    placed = (
        P("query", None),
        P("ctx", "query"),
        P("ctx", "query"),
        P("ctx"),
        P(),
        P("ctx"),
        P("query", None),
    )

    return jax.shard_map(
        local,
        mesh=mesh,
        in_specs=placed,
        out_specs=(
            P(("query", "ctx"), None),
            P(("query", "ctx"), None),
            P("ctx", "query"),
            P("ctx", "query"),
        ),
        check_vma=False,
    )
```

```python
import functools
import math

import jax
import jax.numpy as jnp
from jax import lax
from jax.experimental import pallas as pl
from jax.experimental.pallas import tpu as pltpu
from jax.sharding import PartitionSpec as P


F32 = jnp.float32
BF16 = jnp.bfloat16
MIB = 1024 * 1024
VMEM = pl.BlockSpec(memory_space=pltpu.VMEM)
HBM = pl.BlockSpec(memory_space=pltpu.HBM)


def call(body, out_shape, vmem_mib, flops, **kwargs):
    return pl.pallas_call(
        body,
        out_shape=out_shape,
        compiler_params=pltpu.CompilerParams(vmem_limit_bytes=vmem_mib * MIB),
        cost_estimate=pl.CostEstimate(flops=flops, bytes_accessed=MIB, transcendentals=0),
        **kwargs,
    )


def nt(a, b):
    return lax.dot_general(a, b, (((1,), (1,)), ((), ())), preferred_element_type=F32)


def nn(a, b):
    return lax.dot_general(a, b, (((1,), (0,)), ((), ())), preferred_element_type=F32)


class Plan:
    def __init__(self, query_states, key_states, level_bias):
        self.query_ways = lax.axis_size("query")
        self.owner_ways = lax.axis_size("ctx")
        self.slots, self.features = key_states.shape
        self.heads = level_bias.shape[1] // self.query_ways
        self.head_size = self.features // self.heads
        self.scale = 1.0 / math.sqrt(self.head_size)
        self.own_rows = query_states.shape[0]
        self.rows = self.own_rows * self.query_ways
        self.part_rows = self.own_rows // self.owner_ways
        self.last_rows = self.part_rows * self.query_ways
        self.group = 2 if self.heads % 2 == 0 and self.rows <= 128 else 1
        self.groups = self.heads // self.group
        self.lanes = self.group * self.rows
        self.rounds = self.owner_ways.bit_length() - 1
        assert 1 << self.rounds == self.owner_ways and self.groups <= 8
        counts = [self.rows]
        for _ in range(self.rounds):
            half = counts[-1] // 2
            counts.append(half if half >= 8 else counts[-1])
        self.counts = counts
        self.packed = None
        if self.rounds and counts[-2] == counts[-1] == 8 and self.rows >> self.rounds == 4 and self.group == 2:
            self.packed = self.rounds - 1

    def split(self, k):
        return k < self.rounds and self.counts[k + 1] < self.counts[k]

    def sent_heads(self, k):
        return self.heads // 2 if k == self.packed else self.heads

    def swapped(self, k):
        return 3 - k if self.rounds >= 3 and k in (1, 2) else k

    def bit(self, k):
        owner = lax.axis_index("ctx")
        return (owner >> jnp.where(owner % 2 == 1, self.swapped(k), k)) & 1

    def swap(self, k):
        return [
            (i, i ^ (1 << (self.swapped(k) if i % 2 else k))) for i in range(self.owner_ways)
        ]

    def keep(self, k):
        return self.bit(k) * self.counts[k + 1] if self.split(k) else 0

    def give(self, k):
        return (1 - self.bit(k)) * self.counts[k + 1] if self.split(k) else 0

    def base(self, k):
        return sum((self.keep(j) for j in range(k)), 0)

    def last_offset(self):
        offset = 0
        for k in range(self.rounds):
            if not self.split(k) and k != self.packed:
                offset = offset + self.bit(k) * (self.rows >> (k + 1))
        return offset


def aligned(x, by):
    return pl.multiple_of(x, by) if by >= 8 and not isinstance(x, int) else x


def halves(first, second, upper):
    top = lax.broadcasted_iota(jnp.int32, first.shape, 0) < 4
    lower_rows = jnp.where(top, first, pltpu.roll(second, 4, 0))
    upper_rows = jnp.where(top, pltpu.roll(first, 4, 0), second)
    return jnp.where(upper == 1, upper_rows, lower_rows)


def copy_all(pairs, semaphores):
    copies = [
        pltpu.make_async_copy(source, target, semaphores.at[n]) for n, (source, target) in enumerate(pairs)
    ]
    for copy in copies:
        copy.start()
    return copies


def columns_at(plan, ref, at):
    return ref.at[:, pl.ds(pl.multiple_of(at * plan.features, 128), plan.features)]


def cut_body(plan, q_ref, g_ref, their_q_ref, their_g_ref, semaphores):
    at = 1 - lax.axis_index("query")
    pairs = [(columns_at(plan, q_ref, at), their_q_ref), (columns_at(plan, g_ref, at), their_g_ref)]
    for copy in copy_all(pairs, semaphores):
        copy.wait()


def load_body(plan, pairwise, live_ref, *refs):
    count = 6 if pairwise else 4
    ids_hbm, bias_hbm, k_hbm, v_hbm, *rows_hbm = refs[:count]
    k_ref, v_ref, *rows_refs, term_ref, ids_ref, bias_ref, semaphores = refs[count:]
    me = lax.axis_index("query")
    copies = copy_all(
        [
            (ids_hbm, ids_ref),
            (bias_hbm, bias_ref),
            (k_hbm, k_ref),
            (v_hbm, v_ref),
            *((columns_at(plan, source, me), target) for source, target in zip(rows_hbm, rows_refs)),
        ],
        semaphores,
    )
    for copy in copies[:2]:
        copy.wait()
    ids = ids_ref[...]
    live = lax.broadcasted_iota(jnp.int32, ids.shape, 1) < live_ref[0]
    masks = [ids == level for level in range(bias_ref.shape[0])]
    for h in range(plan.heads):
        row = jnp.zeros(ids.shape, F32)
        for level, mask in enumerate(masks):
            row = jnp.where(mask, bias_ref[level, me * plan.heads + h], row)
        term_ref[h : h + 1, :] = jnp.where(live, row, -1e30)
    for copy in copies[2:]:
        copy.wait()


def row_order(plan):
    rows = plan.rows
    place = lax.broadcasted_iota(jnp.int32, (rows, rows), 0)
    column = lax.broadcasted_iota(jnp.int32, (rows, rows), 1)
    inner = place % plan.last_rows
    outer = place // plan.last_rows
    owner = jnp.zeros_like(outer)
    for k in range(plan.rounds):
        bit = (outer >> (plan.rounds - 1 - k)) & 1
        odd = (outer >> (plan.rounds - 1)) & 1
        owner = owner | (bit << jnp.where(odd == 1, plan.swapped(k), k))
    wanted = (
        inner // plan.part_rows * plan.own_rows + owner * plan.part_rows + inner % plan.part_rows
    )
    return (column == wanted).astype(F32).astype(BF16)


def place_rows(plan, own_ref, moved_ref, block_ref, source):
    rows, size = plan.rows, plan.head_size
    width = plan.group * size
    if own_ref is None:
        source[...] = moved_ref[...]
    else:
        source[: plan.own_rows] = own_ref[...]
        source[plan.own_rows :] = moved_ref[...]
    if plan.group > 1:
        block_ref[...] = jnp.zeros_like(block_ref)
    permute = row_order(plan)
    for p in range(plan.groups):
        ordered = nn(permute, source[:, p * width : (p + 1) * width]).astype(BF16)
        for q in range(plan.group):
            block_ref[p, q * rows : (q + 1) * rows, q * size : (q + 1) * size] = ordered[
                :, q * size : (q + 1) * size
            ]


STEP = 16
TILE = 256


def pipeline(plan, product, chunk, finish):
    tiles = range(0, plan.slots, TILE)
    for j in tiles:
        product(0, j)
    chunks = range(0, plan.lanes, STEP)
    for p in range(plan.groups):
        pending = [functools.partial(product, p + 1, j) for j in tiles] if p + 1 < plan.groups else []
        if p:
            pending.insert(1, functools.partial(finish, p - 1))
        share = -(-len(pending) // len(chunks)) if pending else 0
        gap = max(1, len(chunks) // max(1, len(pending)))
        for i, r in enumerate(chunks):
            chunk(p, r)
            if i % gap == gap - 1:
                for _ in range(share):
                    if pending:
                        pending.pop(0)()
        for work in pending:
            work()
    finish(plan.groups - 1)


def attend_body(plan, pairwise, *refs):
    own_ref = refs[0] if pairwise else None
    refs = refs[1:] if pairwise else refs
    moved_ref, k_ref, v_ref, term_ref, e_ref, eb_ref, out_ref, columns, block_ref, source, scores = refs
    place_rows(plan, own_ref, moved_ref, block_ref, source)
    rows, size, group = plan.rows, plan.head_size, plan.group
    width = group * size
    columns[...] = jnp.zeros_like(columns)

    def product(p, j):
        keys = k_ref[j : j + TILE, p * width : (p + 1) * width]
        scores[p % 2, :, j : j + TILE] = nt(block_ref[p], keys)

    def chunk(p, r):
        h = p * group + r // rows
        s = scores[p % 2, r : r + STEP] * plan.scale + term_ref[h : h + 1, :]
        top = jnp.max(s, axis=1, keepdims=True)
        e = jnp.exp(s - top)
        e_ref[p, r : r + STEP, :] = e
        eb_ref[p, r : r + STEP, :] = e.astype(BF16)
        columns[r : r + STEP, p : p + 1] = top
        columns[r : r + STEP, 8 + p : 9 + p] = jnp.sum(e, axis=1, keepdims=True)

    def finish(p):
        with_values = nn(eb_ref[p], v_ref[:, p * width : (p + 1) * width])
        for q in range(group):
            at, of = slice(q * rows, (q + 1) * rows), slice(q * size, (q + 1) * size)
            out_ref[p * group + q] = with_values[at, of]

    pipeline(plan, product, chunk, finish)


def differ_body(plan, pairwise, *refs):
    own_ref = refs[0] if pairwise else None
    refs = refs[1:] if pairwise else refs
    moved_ref, k_ref, v_ref, e_ref, eb_ref, out_ref, columns_ref = refs[:7]
    part_ref, send_ref, stat_ref, yb_ref, block_ref, source, dprobs, columns = refs[7:]
    place_rows(plan, own_ref, moved_ref, block_ref, source)
    rows, size, group = plan.rows, plan.head_size, plan.group
    width = group * size
    columns[...] = columns_ref[...]
    part_ref[0] = out_ref[...]

    def product(p, j):
        values = v_ref[j : j + TILE, p * width : (p + 1) * width]
        dprobs[p % 2, :, j : j + TILE] = nt(block_ref[p], values)

    def chunk(p, r):
        e = e_ref[p, r : r + STEP, :]
        d = dprobs[p % 2, r : r + STEP]
        total = columns_ref[r : r + STEP, 8 + p : 9 + p]
        mean = jnp.sum(e * d, axis=1, keepdims=True) / total
        yb_ref[p, r : r + STEP, :] = (e * (d - mean)).astype(BF16)
        columns[r : r + STEP, 16 + p : 17 + p] = mean

    def finish(p):
        both = jnp.concatenate([eb_ref[p], yb_ref[p]], axis=0)
        with_keys = nn(both, k_ref[:, p * width : (p + 1) * width])
        for a in range(2):
            for q in range(group):
                start, of = a * plan.lanes + q * rows, slice(q * size, (q + 1) * size)
                part_ref[1 + a, p * group + q] = with_keys[start : start + rows, of]

    pipeline(plan, product, chunk, finish)
    give(plan, 0, part_ref, send_ref)
    stat_ref[...] = columns[...].T[:24]


def statistics(stat_ref, stat_came_ref):
    top1, total1, mean1 = (stat_ref[8 * t : 8 * t + 8] for t in range(3))
    top2, total2, mean2 = (stat_came_ref[8 * t : 8 * t + 8] for t in range(3))
    top = jnp.maximum(top1, top2)
    f1 = jnp.exp(top1 - top)
    f2 = jnp.exp(top2 - top)
    total = f1 * total1 + f2 * total2
    inverse = 1.0 / jnp.where(total > 0.0, total, 1.0)
    w1 = f1 * total1 * inverse
    w2 = f2 * total2 * inverse
    gap = mean1 - mean2
    merged = (top, total, mean1 * w1 + mean2 * w2)
    return merged, (f1, f2, f1 * w2 * gap, -f2 * w1 * gap, inverse)


def merge_statistics_body(stat_ref, stat_came_ref, stat_new_ref):
    merged, _ = statistics(stat_ref, stat_came_ref)
    for t in range(3):
        stat_new_ref[8 * t : 8 * t + 8] = merged[t]


def merge_body(plan, k, part_ref, came_ref, stat_ref, stat_came_ref, *refs):
    last = k == plan.rounds - 1
    if last:
        own_ref, away_ref, table = refs if len(refs) == 3 else (None, *refs)
    else:
        part_new_ref, send_ref, table = refs
    _, factors = statistics(stat_ref, stat_came_ref)
    rest = jnp.zeros((128 - 40, plan.lanes), F32)
    table[...] = jnp.concatenate([*factors, rest], axis=0).T
    count = plan.counts[k + 1]
    kept = pl.ds(aligned(plan.keep(k), count), count)
    base = plan.base(k + 1)
    rows_of = [pl.ds(aligned(q * plan.rows + base, count), count) for q in range(plan.group)]
    packed = k == plan.packed
    bit = plan.bit(k)
    if packed:
        joined = halves(table[rows_of[0], :], table[rows_of[1], :], bit)
    for n in range(plan.sent_heads(k)):
        if packed:
            p = n
            mine = [halves(part_ref[a, 2 * n], part_ref[a, 2 * n + 1], bit) for a in range(3)]
            rows = joined
        else:
            p = n // plan.group
            mine = [part_ref[a, n, kept, :] for a in range(3)]
            rows = table[rows_of[n % plan.group], :]
        col = lambda t: rows[:, 8 * t + p : 8 * t + p + 1]
        out1, key1, dif1 = mine
        out2, key2, dif2 = (came_ref[a, n].astype(F32) for a in range(3))
        c1, c2 = col(0), col(1)
        out = c1 * out1 + c2 * out2
        dif = c1 * dif1 + c2 * dif2 + col(2) * key1 + col(3) * key2
        if not last:
            part_new_ref[0, n] = out
            part_new_ref[1, n] = c1 * key1 + c2 * key2
            part_new_ref[2, n] = dif
            continue
        share = col(4)
        for a, x in ((0, out * share), (1, dif * (share * plan.scale))):
            offset = plan.last_offset()
            if not isinstance(offset, int):
                x = pltpu.roll(x, (count - offset) % count, 0)
            for h, start in ((2 * n, 0), (2 * n + 1, 4)) if packed else ((n, 0),):
                of = slice(h * plan.head_size, (h + 1) * plan.head_size)
                middle, end = start + plan.part_rows, start + plan.last_rows
                if own_ref is not None:
                    own_ref[a, :, of] = x[start:middle].astype(BF16)
                    away_ref[a, :, of] = x[middle:end].astype(BF16)
                else:
                    away_ref[a, :, of] = x[start:end].astype(BF16)
    if not last:
        give(plan, k + 1, part_new_ref, send_ref)


def give(plan, k, part_ref, send_ref):
    if k == plan.packed:
        for a in range(3):
            for n in range(plan.heads // 2):
                x = halves(part_ref[a, 2 * n], part_ref[a, 2 * n + 1], 1 - plan.bit(k))
                send_ref[a, n] = x.astype(BF16)
        return
    count = plan.counts[k + 1]
    gone = pl.ds(aligned(plan.give(k), count), count)
    for a in range(3):
        for h in range(plan.heads):
            send_ref[a, h] = part_ref[a, h, gone, :].astype(BF16)


def gather_body(plan, own_ref, back_ref, attn_ref, dq_ref):
    me = lax.axis_index("query")
    for a, out_ref in ((0, attn_ref), (1, dq_ref)):
        for at, ref in ((me, own_ref), (1 - me, back_ref)):
            start = pl.multiple_of(at * plan.features, 128)
            out_ref[:, pl.ds(start, plan.features)] = ref[a]


def turn_body(eb_ref, yb_ref, turned_ref):
    lanes = eb_ref.shape[1]
    for p in range(eb_ref.shape[0]):
        turned_ref[p, :, :lanes] = eb_ref[p].T
        turned_ref[p, :, lanes:] = yb_ref[p].T


def backward_body(plan, first, count, stat_ref, stat_all_ref, qb_ref, gb_ref, turned_ref, *refs):
    dk_ref, dv_ref, table, dk, dv, semaphores = refs[-6:]
    lanes = plan.lanes
    width = dk.shape[2]
    total = stat_all_ref[8:16]
    inverse = 1.0 / jnp.where(total > 0.0, total, 1.0)
    f = jnp.exp(stat_ref[0:8] - stat_all_ref[0:8]) * inverse
    c = f * (stat_ref[16:24] - stat_all_ref[16:24])
    rest = jnp.zeros((128 - 24, lanes), F32)
    table[...] = jnp.concatenate([f, f * plan.scale, c * plan.scale, rest], axis=0).T
    copies = []
    for p in range(first, first + count):
        queries = qb_ref[p].astype(F32)
        wv = (gb_ref[p].astype(F32) * table[:, p : p + 1]).astype(BF16)
        wc = (queries * table[:, 16 + p : 17 + p]).astype(BF16)
        wf = (queries * table[:, 8 + p : 9 + p]).astype(BF16)
        for n, (buffer, target) in enumerate(((dk, dk_ref), (dv, dv_ref))):
            if n == 0:
                buffer[p - first] = nn(turned_ref[p], jnp.concatenate([wc, wf], axis=0)).astype(BF16)
            else:
                buffer[p - first] = nn(turned_ref[p, :, :lanes], wv).astype(BF16)
            copy = pltpu.make_async_copy(
                buffer.at[p - first], target.at[:, p * width : (p + 1) * width], semaphores.at[n, p - first]
            )
            copy.start()
            copies.append(copy)
    for copy in copies:
        copy.wait()


def local(query_states, key_states, value_states, level_ids, level_bias, live_counts, out_grad):
    plan = Plan(query_states, key_states, level_bias)
    size, slots, lanes, groups, heads = plan.head_size, plan.slots, plan.lanes, plan.groups, plan.heads
    width = plan.group * size
    pairwise = plan.query_ways == 2
    own_shape = jax.ShapeDtypeStruct((plan.own_rows, plan.features), BF16)
    pairwise = plan.query_ways == 2
    in_hbm = lambda arrays: [pltpu.with_memory_space_constraint(x, pltpu.HBM) for x in arrays]
    if pairwise:
        their_queries, their_grads = call(
            functools.partial(cut_body, plan),
            [own_shape] * 2,
            2,
            10**6,
            in_specs=[HBM] * 2,
            out_specs=[VMEM] * 2,
            scratch_shapes=[pltpu.SemaphoreType.DMA((2,))],
            name="cut",
        )(*in_hbm([query_states, out_grad]))
        moved_queries = lax.ppermute(their_queries, "query", [(0, 1), (1, 0)])
        moved_grads = lax.ppermute(their_grads, "query", [(0, 1), (1, 0)])
    else:
        moved_queries, moved_grads = (
            lax.all_to_all(x, "query", split_axis=1, concat_axis=0, tiled=True)
            for x in (query_states, out_grad)
        )

    stat_shape = jax.ShapeDtypeStruct((24, lanes), F32)
    block_shape = jax.ShapeDtypeStruct((groups, lanes, width), BF16)
    square_shape = lambda dtype: jax.ShapeDtypeStruct((groups, lanes, slots), dtype)
    part_shape = lambda k: jax.ShapeDtypeStruct((3, heads, plan.counts[k], size), F32)
    send_shape = lambda k: jax.ShapeDtypeStruct(
        (3, plan.sent_heads(k), plan.counts[k + 1], size), BF16
    )
    context_shape = jax.ShapeDtypeStruct(key_states.shape, BF16)
    columns_shape = jax.ShapeDtypeStruct((lanes, 128), F32)
    source_scratch = pltpu.VMEM((plan.rows, plan.features), BF16)
    square_scratch = pltpu.VMEM((2, lanes, slots), F32)

    def kernel(name, body, outs, ins, scratch, vmem_mib=4, flops=10**9):
        single = not isinstance(outs, (tuple, list))
        return call(
            body,
            outs,
            vmem_mib,
            flops,
            in_specs=[VMEM] * len(ins),
            out_specs=VMEM if single else [VMEM] * len(outs),
            scratch_shapes=scratch,
            name=name,
        )(*ins)

    from_hbm = [level_ids.reshape(1, slots), level_bias, key_states, value_states]
    from_hbm += [query_states, out_grad] if pairwise else []
    own_shapes = [own_shape] * 2 if pairwise else []
    keys, values, *own, term = call(
        functools.partial(load_body, plan, pairwise),
        [context_shape] * 2 + own_shapes + [jax.ShapeDtypeStruct((heads, slots), F32)],
        2,
        10**9,
        in_specs=[pl.BlockSpec(memory_space=pltpu.SMEM)] + [HBM] * len(from_hbm),
        out_specs=[VMEM] * (3 + len(own_shapes)),
        scratch_shapes=[
            pltpu.VMEM((1, slots), jnp.int32),
            pltpu.SMEM(level_bias.shape, F32),
            pltpu.SemaphoreType.DMA((len(from_hbm),)),
        ],
        name="load",
    )(live_counts, *in_hbm(from_hbm))
    own_queries, own_grads = ([own[0]], [own[1]]) if pairwise else ([], [])
    e, eb, out, columns, qb = kernel(
        "attend",
        functools.partial(attend_body, plan, pairwise),
        (
            square_shape(F32),
            square_shape(BF16),
            jax.ShapeDtypeStruct((heads, plan.rows, size), F32),
            columns_shape,
            block_shape,
        ),
        (*own_queries, moved_queries, keys, values, term),
        [source_scratch, square_scratch],
        vmem_mib=6,
    )
    part, send, stat_own, yb, gb = kernel(
        "differ",
        functools.partial(differ_body, plan, pairwise),
        (part_shape(0), send_shape(0), stat_shape, square_shape(BF16), block_shape),
        (*own_grads, moved_grads, keys, values, e, eb, out, columns),
        [source_scratch, square_scratch, pltpu.VMEM((lanes, 128), F32)],
        vmem_mib=6,
    )
    turned = kernel(
        "turn", turn_body, jax.ShapeDtypeStruct((groups, slots, 2 * lanes), BF16), (eb, yb), []
    )

    stat = stat_own
    for k in range(plan.rounds):
        swap = plan.swap(k)
        stat_came = lax.ppermute(stat, "ctx", swap)
        came = lax.ppermute(send, "ctx", swap)
        merged = call(
            merge_statistics_body,
            stat_shape,
            2,
            10**6,
            in_specs=[VMEM] * 2,
            out_specs=VMEM,
            name=f"statistics{k}",
        )(stat, stat_came)
        if k < plan.rounds - 1:
            outs = (part_shape(k + 1), send_shape(k + 1))
        elif pairwise:
            outs = (jax.ShapeDtypeStruct((2, plan.part_rows, plan.features), BF16),) * 2
        else:
            outs = (jax.ShapeDtypeStruct((2, plan.last_rows, plan.features), BF16),)
        part, send, *_ = call(
            functools.partial(merge_body, plan, k),
            outs,
            4,
            10**8,
            in_specs=[VMEM] * 4,
            out_specs=[VMEM] * len(outs),
            scratch_shapes=[pltpu.VMEM((lanes, 128), F32)],
            name=f"merge{k}",
        )(part, came, stat, stat_came) + (None,) * (2 - len(outs))
        stat = merged
    if pairwise:
        own, away = part, send
        back = lax.ppermute(away, "query", [(0, 1), (1, 0)])

    def gradients(name, first, count, *into):
        return call(
            functools.partial(backward_body, plan, first, count),
            (context_shape, context_shape),
            8,
            4 * 10**9,
            in_specs=[VMEM] * 5 + [HBM] * len(into),
            out_specs=[HBM] * 2,
            scratch_shapes=[
                pltpu.VMEM((lanes, 128), F32),
                pltpu.VMEM((count, slots, width), BF16),
                pltpu.VMEM((count, slots, width), BF16),
                pltpu.SemaphoreType.DMA((2, count)),
            ],
            input_output_aliases={5 + n: n for n in range(len(into))},
            name=name,
        )(stat_own, stat, qb, gb, turned, *into)

    split = (groups + 1) // 2
    grads = gradients("backward0", 0, split)
    key_grad, value_grad = gradients("backward1", split, groups - split, *grads)

    if not pairwise:
        final = lax.all_to_all(part, "query", split_axis=1, concat_axis=2, tiled=True)
        return final[0], final[1], key_grad, value_grad
    whole_rows = jax.ShapeDtypeStruct((plan.part_rows, 2 * plan.features), BF16)
    attn, query_grad = kernel(
        "gather", functools.partial(gather_body, plan), (whole_rows, whole_rows), (own, back), []
    )
    return attn, query_grad, key_grad, value_grad


def solution(mesh):
    placed = (
        P("query", None),
        P("ctx", "query"),
        P("ctx", "query"),
        P("ctx"),
        P(),
        P("ctx"),
        P("query", None),
    )

    return jax.shard_map(
        local,
        mesh=mesh,
        in_specs=placed,
        out_specs=(
            P(("query", "ctx"), None),
            P(("query", "ctx"), None),
            P("ctx", "query"),
            P("ctx", "query"),
        ),
        check_vma=False,
    )
```

```python
import functools
import math

import jax
import jax.numpy as jnp
from jax import lax
from jax.experimental import pallas as pl
from jax.experimental.pallas import tpu as pltpu
from jax.sharding import PartitionSpec as P


F32 = jnp.float32
BF16 = jnp.bfloat16
MIB = 1024 * 1024
VMEM = pl.BlockSpec(memory_space=pltpu.VMEM)
HBM = pl.BlockSpec(memory_space=pltpu.HBM)


def call(body, out_shape, vmem_mib, flops, **kwargs):
    return pl.pallas_call(
        body,
        out_shape=out_shape,
        compiler_params=pltpu.CompilerParams(vmem_limit_bytes=vmem_mib * MIB),
        cost_estimate=pl.CostEstimate(flops=flops, bytes_accessed=MIB, transcendentals=0),
        **kwargs,
    )


def nt(a, b):
    return lax.dot_general(a, b, (((1,), (1,)), ((), ())), preferred_element_type=F32)


def nn(a, b):
    return lax.dot_general(a, b, (((1,), (0,)), ((), ())), preferred_element_type=F32)


class Plan:
    def __init__(self, query_states, key_states, level_bias):
        self.query_ways = lax.axis_size("query")
        self.owner_ways = lax.axis_size("ctx")
        self.slots, self.features = key_states.shape
        self.heads = level_bias.shape[1] // self.query_ways
        self.head_size = self.features // self.heads
        self.scale = 1.0 / math.sqrt(self.head_size)
        self.own_rows = query_states.shape[0]
        self.rows = self.own_rows * self.query_ways
        self.part_rows = self.own_rows // self.owner_ways
        self.last_rows = self.part_rows * self.query_ways
        self.group = 2 if self.heads % 2 == 0 and self.rows <= 128 else 1
        self.groups = self.heads // self.group
        self.lanes = self.group * self.rows
        self.rounds = self.owner_ways.bit_length() - 1
        assert 1 << self.rounds == self.owner_ways and self.groups <= 8
        counts = [self.rows]
        for _ in range(self.rounds):
            half = counts[-1] // 2
            counts.append(half if half >= 8 else counts[-1])
        self.counts = counts
        self.packed = None
        if self.rounds and counts[-2] == counts[-1] == 8 and self.rows >> self.rounds == 4 and self.group == 2:
            self.packed = self.rounds - 1

    def split(self, k):
        return k < self.rounds and self.counts[k + 1] < self.counts[k]

    def sent_heads(self, k):
        return self.heads // 2 if k == self.packed else self.heads

    def swapped(self, k):
        return 3 - k if self.rounds >= 3 and k in (1, 2) else k

    def bit(self, k):
        owner = lax.axis_index("ctx")
        return (owner >> jnp.where(owner % 2 == 1, self.swapped(k), k)) & 1

    def swap(self, k):
        return [
            (i, i ^ (1 << (self.swapped(k) if i % 2 else k))) for i in range(self.owner_ways)
        ]

    def keep(self, k):
        return self.bit(k) * self.counts[k + 1] if self.split(k) else 0

    def give(self, k):
        return (1 - self.bit(k)) * self.counts[k + 1] if self.split(k) else 0

    def base(self, k):
        return sum((self.keep(j) for j in range(k)), 0)

    def last_offset(self):
        offset = 0
        for k in range(self.rounds):
            if not self.split(k) and k != self.packed:
                offset = offset + self.bit(k) * (self.rows >> (k + 1))
        return offset


def aligned(x, by):
    return pl.multiple_of(x, by) if by >= 8 and not isinstance(x, int) else x


def halves(first, second, upper):
    top = lax.broadcasted_iota(jnp.int32, first.shape, 0) < 4
    lower_rows = jnp.where(top, first, pltpu.roll(second, 4, 0))
    upper_rows = jnp.where(top, pltpu.roll(first, 4, 0), second)
    return jnp.where(upper == 1, upper_rows, lower_rows)


def copy_all(pairs, semaphores):
    copies = [
        pltpu.make_async_copy(source, target, semaphores.at[n]) for n, (source, target) in enumerate(pairs)
    ]
    for copy in copies:
        copy.start()
    return copies


def columns_at(plan, ref, at):
    return ref.at[:, pl.ds(pl.multiple_of(at * plan.features, 128), plan.features)]


def cut_body(plan, q_ref, g_ref, their_q_ref, their_g_ref, semaphores):
    at = 1 - lax.axis_index("query")
    pairs = [(columns_at(plan, q_ref, at), their_q_ref), (columns_at(plan, g_ref, at), their_g_ref)]
    for copy in copy_all(pairs, semaphores):
        copy.wait()


def load_body(plan, pairwise, *refs):
    count = 6 if pairwise else 4
    ids_hbm, bias_hbm, k_hbm, v_hbm, *rows_hbm = refs[:count]
    k_ref, v_ref, kt_ref, *rows_refs, term_ref, ids_ref, bias_ref, semaphores = refs[count:]
    me = lax.axis_index("query")
    pieces = [slice(j, j + PIECE) for j in range(0, plan.slots, PIECE)]
    parts = [(k_hbm, k_ref, kt_ref, of) for of in pieces] + [(v_hbm, v_ref, None, of) for of in pieces]
    copies = copy_all(
        [
            (ids_hbm, ids_ref),
            (bias_hbm, bias_ref),
            *((source.at[of], target.at[of]) for source, target, _, of in parts),
            *((columns_at(plan, source, me), target) for source, target in zip(rows_hbm, rows_refs)),
        ],
        semaphores,
    )
    for copy in copies[:2]:
        copy.wait()
    ids = ids_ref[...]
    masks = [ids == level for level in range(bias_ref.shape[0])]
    for h in range(plan.heads):
        row = jnp.zeros(ids.shape, F32)
        for level, mask in enumerate(masks):
            row = jnp.where(mask, bias_ref[level, me * plan.heads + h], row)
        term_ref[h : h + 1, :] = row
    for copy, (_, target, turned, of) in zip(copies[2:], parts):
        copy.wait()
        if turned is not None:
            turned[:, of] = target[of].T
    for copy in copies[2 + len(parts) :]:
        copy.wait()


def mask_body(live_ref, term_ref, masked_ref):
    slot = lax.broadcasted_iota(jnp.int32, term_ref.shape, 1)
    masked_ref[...] = jnp.where(slot < live_ref[0], term_ref[...], -1e30)


def row_order(plan):
    rows = plan.rows
    place = lax.broadcasted_iota(jnp.int32, (rows, rows), 0)
    column = lax.broadcasted_iota(jnp.int32, (rows, rows), 1)
    inner = place % plan.last_rows
    outer = place // plan.last_rows
    owner = jnp.zeros_like(outer)
    for k in range(plan.rounds):
        bit = (outer >> (plan.rounds - 1 - k)) & 1
        odd = (outer >> (plan.rounds - 1)) & 1
        owner = owner | (bit << jnp.where(odd == 1, plan.swapped(k), k))
    wanted = (
        inner // plan.part_rows * plan.own_rows + owner * plan.part_rows + inner % plan.part_rows
    )
    return (column == wanted).astype(F32).astype(BF16)


def place_rows(plan, own_ref, moved_ref, block_ref, source):
    rows, size = plan.rows, plan.head_size
    width = plan.group * size
    if own_ref is None:
        source[...] = moved_ref[...]
    else:
        source[: plan.own_rows] = own_ref[...]
        source[plan.own_rows :] = moved_ref[...]
    if plan.group > 1:
        block_ref[...] = jnp.zeros_like(block_ref)
    permute = row_order(plan)
    for p in range(plan.groups):
        ordered = nn(permute, source[:, p * width : (p + 1) * width]).astype(BF16)
        for q in range(plan.group):
            block_ref[p, q * rows : (q + 1) * rows, q * size : (q + 1) * size] = ordered[
                :, q * size : (q + 1) * size
            ]


STEP = 16
PIECE = 256
TILE = 256


def pipeline(plan, product, chunk, finish):
    tiles = range(0, plan.slots, TILE)
    for j in tiles:
        product(0, j)
    chunks = range(0, plan.lanes, STEP)
    for p in range(plan.groups):
        pending = [functools.partial(product, p + 1, j) for j in tiles] if p + 1 < plan.groups else []
        if p:
            pending.insert(1, functools.partial(finish, p - 1))
        share = -(-len(pending) // len(chunks)) if pending else 0
        gap = max(1, len(chunks) // max(1, len(pending)))
        for i, r in enumerate(chunks):
            chunk(p, r)
            if i % gap == gap - 1:
                for _ in range(share):
                    if pending:
                        pending.pop(0)()
        for work in pending:
            work()
    finish(plan.groups - 1)


def attend_body(plan, pairwise, *refs):
    own_ref = refs[0] if pairwise else None
    refs = refs[1:] if pairwise else refs
    moved_ref, kt_ref, v_ref, term_ref, e_ref, eb_ref, out_ref, columns, block_ref, source, scores = refs
    place_rows(plan, own_ref, moved_ref, block_ref, source)
    rows, size, group = plan.rows, plan.head_size, plan.group
    width = group * size
    columns[...] = jnp.zeros_like(columns)

    def product(p, j):
        scores[p % 2, :, j : j + TILE] = nn(block_ref[p], kt_ref[p * width : (p + 1) * width, j : j + TILE])

    def chunk(p, r):
        h = p * group + r // rows
        s = scores[p % 2, r : r + STEP] * plan.scale + term_ref[h : h + 1, :]
        top = jnp.max(s, axis=1, keepdims=True)
        e = jnp.exp(s - top)
        e_ref[p, r : r + STEP, :] = e
        eb_ref[p, r : r + STEP, :] = e.astype(BF16)
        columns[r : r + STEP, p : p + 1] = top
        columns[r : r + STEP, 8 + p : 9 + p] = jnp.sum(e, axis=1, keepdims=True)

    def finish(p):
        with_values = nn(eb_ref[p], v_ref[:, p * width : (p + 1) * width])
        for q in range(group):
            at, of = slice(q * rows, (q + 1) * rows), slice(q * size, (q + 1) * size)
            out_ref[p * group + q] = with_values[at, of]

    pipeline(plan, product, chunk, finish)


def differ_body(plan, pairwise, *refs):
    own_ref = refs[0] if pairwise else None
    refs = refs[1:] if pairwise else refs
    moved_ref, k_ref, vt_ref, e_ref, eb_ref, out_ref, columns_ref = refs[:7]
    part_ref, send_ref, stat_ref, yb_ref, block_ref, source, dprobs, columns = refs[7:]
    place_rows(plan, own_ref, moved_ref, block_ref, source)
    rows, size, group = plan.rows, plan.head_size, plan.group
    width = group * size
    columns[...] = columns_ref[...]
    part_ref[0] = out_ref[...]

    def product(p, j):
        dprobs[p % 2, :, j : j + TILE] = nt(block_ref[p], vt_ref[j : j + TILE, p * width : (p + 1) * width])

    def chunk(p, r):
        e = e_ref[p, r : r + STEP, :]
        d = dprobs[p % 2, r : r + STEP]
        total = columns_ref[r : r + STEP, 8 + p : 9 + p]
        mean = jnp.sum(e * d, axis=1, keepdims=True) / total
        yb_ref[p, r : r + STEP, :] = (e * (d - mean)).astype(BF16)
        columns[r : r + STEP, 16 + p : 17 + p] = mean

    def finish(p):
        both = jnp.concatenate([eb_ref[p], yb_ref[p]], axis=0)
        with_keys = nn(both, k_ref[:, p * width : (p + 1) * width])
        for a in range(2):
            for q in range(group):
                start, of = a * plan.lanes + q * rows, slice(q * size, (q + 1) * size)
                part_ref[1 + a, p * group + q] = with_keys[start : start + rows, of]

    pipeline(plan, product, chunk, finish)
    give(plan, 0, part_ref, send_ref)
    stat_ref[...] = columns[...].T[:24]


def statistics(stat_ref, stat_came_ref):
    top1, total1, mean1 = (stat_ref[8 * t : 8 * t + 8] for t in range(3))
    top2, total2, mean2 = (stat_came_ref[8 * t : 8 * t + 8] for t in range(3))
    top = jnp.maximum(top1, top2)
    f1 = jnp.exp(top1 - top)
    f2 = jnp.exp(top2 - top)
    total = f1 * total1 + f2 * total2
    inverse = 1.0 / jnp.where(total > 0.0, total, 1.0)
    w1 = f1 * total1 * inverse
    w2 = f2 * total2 * inverse
    gap = mean1 - mean2
    merged = (top, total, mean1 * w1 + mean2 * w2)
    return merged, (f1, f2, f1 * w2 * gap, -f2 * w1 * gap, inverse)


def merge_statistics_body(stat_ref, stat_came_ref, stat_new_ref):
    merged, _ = statistics(stat_ref, stat_came_ref)
    for t in range(3):
        stat_new_ref[8 * t : 8 * t + 8] = merged[t]


def merge_body(plan, k, part_ref, came_ref, stat_ref, stat_came_ref, *refs):
    last = k == plan.rounds - 1
    if last:
        own_ref, away_ref, table = refs if len(refs) == 3 else (None, *refs)
    else:
        part_new_ref, send_ref, table = refs
    _, factors = statistics(stat_ref, stat_came_ref)
    rest = jnp.zeros((128 - 40, plan.lanes), F32)
    table[...] = jnp.concatenate([*factors, rest], axis=0).T
    count = plan.counts[k + 1]
    kept = pl.ds(aligned(plan.keep(k), count), count)
    base = plan.base(k + 1)
    rows_of = [pl.ds(aligned(q * plan.rows + base, count), count) for q in range(plan.group)]
    packed = k == plan.packed
    bit = plan.bit(k)
    if packed:
        joined = halves(table[rows_of[0], :], table[rows_of[1], :], bit)
    for n in range(plan.sent_heads(k)):
        if packed:
            p = n
            mine = [halves(part_ref[a, 2 * n], part_ref[a, 2 * n + 1], bit) for a in range(3)]
            rows = joined
        else:
            p = n // plan.group
            mine = [part_ref[a, n, kept, :] for a in range(3)]
            rows = table[rows_of[n % plan.group], :]
        col = lambda t: rows[:, 8 * t + p : 8 * t + p + 1]
        out1, key1, dif1 = mine
        out2, key2, dif2 = (came_ref[a, n].astype(F32) for a in range(3))
        c1, c2 = col(0), col(1)
        out = c1 * out1 + c2 * out2
        dif = c1 * dif1 + c2 * dif2 + col(2) * key1 + col(3) * key2
        if not last:
            part_new_ref[0, n] = out
            part_new_ref[1, n] = c1 * key1 + c2 * key2
            part_new_ref[2, n] = dif
            continue
        share = col(4)
        for a, x in ((0, out * share), (1, dif * (share * plan.scale))):
            offset = plan.last_offset()
            if not isinstance(offset, int):
                x = pltpu.roll(x, (count - offset) % count, 0)
            for h, start in ((2 * n, 0), (2 * n + 1, 4)) if packed else ((n, 0),):
                of = slice(h * plan.head_size, (h + 1) * plan.head_size)
                middle, end = start + plan.part_rows, start + plan.last_rows
                if own_ref is not None:
                    own_ref[a, :, of] = x[start:middle].astype(BF16)
                    away_ref[a, :, of] = x[middle:end].astype(BF16)
                else:
                    away_ref[a, :, of] = x[start:end].astype(BF16)
    if not last:
        give(plan, k + 1, part_new_ref, send_ref)


def give(plan, k, part_ref, send_ref):
    if k == plan.packed:
        for a in range(3):
            for n in range(plan.heads // 2):
                x = halves(part_ref[a, 2 * n], part_ref[a, 2 * n + 1], 1 - plan.bit(k))
                send_ref[a, n] = x.astype(BF16)
        return
    count = plan.counts[k + 1]
    gone = pl.ds(aligned(plan.give(k), count), count)
    for a in range(3):
        for h in range(plan.heads):
            send_ref[a, h] = part_ref[a, h, gone, :].astype(BF16)


def gather_body(plan, own_ref, back_ref, attn_ref, dq_ref):
    me = lax.axis_index("query")
    for a, out_ref in ((0, attn_ref), (1, dq_ref)):
        for at, ref in ((me, own_ref), (1 - me, back_ref)):
            start = pl.multiple_of(at * plan.features, 128)
            out_ref[:, pl.ds(start, plan.features)] = ref[a]


def turn_body(eb_ref, yb_ref, turned_ref):
    lanes = eb_ref.shape[1]
    for p in range(eb_ref.shape[0]):
        turned_ref[p, :, :lanes] = eb_ref[p].T
        turned_ref[p, :, lanes:] = yb_ref[p].T


def backward_body(plan, first, count, stat_ref, stat_all_ref, qb_ref, gb_ref, turned_ref, *refs):
    dk_ref, dv_ref, table, dk, dv, semaphores = refs[-6:]
    lanes = plan.lanes
    width = dk.shape[2]
    total = stat_all_ref[8:16]
    inverse = 1.0 / jnp.where(total > 0.0, total, 1.0)
    f = jnp.exp(stat_ref[0:8] - stat_all_ref[0:8]) * inverse
    c = f * (stat_ref[16:24] - stat_all_ref[16:24])
    rest = jnp.zeros((128 - 24, lanes), F32)
    table[...] = jnp.concatenate([f, f * plan.scale, c * plan.scale, rest], axis=0).T
    copies = []
    for p in range(first, first + count):
        queries = qb_ref[p].astype(F32)
        wv = (gb_ref[p].astype(F32) * table[:, p : p + 1]).astype(BF16)
        wc = (queries * table[:, 16 + p : 17 + p]).astype(BF16)
        wf = (queries * table[:, 8 + p : 9 + p]).astype(BF16)
        for n, (buffer, target) in enumerate(((dk, dk_ref), (dv, dv_ref))):
            if n == 0:
                buffer[p - first] = nn(turned_ref[p], jnp.concatenate([wc, wf], axis=0)).astype(BF16)
            else:
                buffer[p - first] = nn(turned_ref[p, :, :lanes], wv).astype(BF16)
            copy = pltpu.make_async_copy(
                buffer.at[p - first], target.at[:, p * width : (p + 1) * width], semaphores.at[n, p - first]
            )
            copy.start()
            copies.append(copy)
    for copy in copies:
        copy.wait()


def local(query_states, key_states, value_states, level_ids, level_bias, live_counts, out_grad):
    plan = Plan(query_states, key_states, level_bias)
    size, slots, lanes, groups, heads = plan.head_size, plan.slots, plan.lanes, plan.groups, plan.heads
    width = plan.group * size
    pairwise = plan.query_ways == 2
    own_shape = jax.ShapeDtypeStruct((plan.own_rows, plan.features), BF16)
    pairwise = plan.query_ways == 2
    in_hbm = lambda arrays: [pltpu.with_memory_space_constraint(x, pltpu.HBM) for x in arrays]
    if pairwise:
        their_queries, their_grads = call(
            functools.partial(cut_body, plan),
            [own_shape] * 2,
            2,
            10**6,
            in_specs=[HBM] * 2,
            out_specs=[VMEM] * 2,
            scratch_shapes=[pltpu.SemaphoreType.DMA((2,))],
            name="cut",
        )(*in_hbm([query_states, out_grad]))
        moved_queries = lax.ppermute(their_queries, "query", [(0, 1), (1, 0)])
        moved_grads = lax.ppermute(their_grads, "query", [(0, 1), (1, 0)])
    else:
        moved_queries, moved_grads = (
            lax.all_to_all(x, "query", split_axis=1, concat_axis=0, tiled=True)
            for x in (query_states, out_grad)
        )

    stat_shape = jax.ShapeDtypeStruct((24, lanes), F32)
    block_shape = jax.ShapeDtypeStruct((groups, lanes, width), BF16)
    square_shape = lambda dtype: jax.ShapeDtypeStruct((groups, lanes, slots), dtype)
    part_shape = lambda k: jax.ShapeDtypeStruct((3, heads, plan.counts[k], size), F32)
    send_shape = lambda k: jax.ShapeDtypeStruct(
        (3, plan.sent_heads(k), plan.counts[k + 1], size), BF16
    )
    context_shape = jax.ShapeDtypeStruct(key_states.shape, BF16)
    columns_shape = jax.ShapeDtypeStruct((lanes, 128), F32)
    source_scratch = pltpu.VMEM((plan.rows, plan.features), BF16)
    square_scratch = pltpu.VMEM((2, lanes, slots), F32)

    def kernel(name, body, outs, ins, scratch, vmem_mib=4, flops=10**9):
        single = not isinstance(outs, (tuple, list))
        return call(
            body,
            outs,
            vmem_mib,
            flops,
            in_specs=[VMEM] * len(ins),
            out_specs=VMEM if single else [VMEM] * len(outs),
            scratch_shapes=scratch,
            name=name,
        )(*ins)

    from_hbm = [level_ids.reshape(1, slots), level_bias, key_states, value_states]
    from_hbm += [query_states, out_grad] if pairwise else []
    own_shapes = [own_shape] * 2 if pairwise else []
    turned_shape = jax.ShapeDtypeStruct((plan.features, slots), BF16)
    term_shape = jax.ShapeDtypeStruct((heads, slots), F32)
    keys, values, keys_turned, *own, term = call(
        functools.partial(load_body, plan, pairwise),
        [context_shape] * 2 + [turned_shape] + own_shapes + [term_shape],
        4,
        10**9,
        in_specs=[HBM] * len(from_hbm),
        out_specs=[VMEM] * (4 + len(own_shapes)),
        scratch_shapes=[
            pltpu.VMEM((1, slots), jnp.int32),
            pltpu.SMEM(level_bias.shape, F32),
            pltpu.SemaphoreType.DMA((len(from_hbm) - 2 + 2 * slots // PIECE,)),
        ],
        name="load",
    )(*in_hbm(from_hbm))
    term = call(
        mask_body,
        term_shape,
        2,
        10**6,
        in_specs=[pl.BlockSpec(memory_space=pltpu.SMEM), VMEM],
        out_specs=VMEM,
        name="mask",
    )(live_counts, term)
    own_queries, own_grads = ([own[0]], [own[1]]) if pairwise else ([], [])
    e, eb, out, columns, qb = kernel(
        "attend",
        functools.partial(attend_body, plan, pairwise),
        (
            square_shape(F32),
            square_shape(BF16),
            jax.ShapeDtypeStruct((heads, plan.rows, size), F32),
            columns_shape,
            block_shape,
        ),
        (*own_queries, moved_queries, keys_turned, values, term),
        [source_scratch, square_scratch],
        vmem_mib=6,
    )
    part, send, stat_own, yb, gb = kernel(
        "differ",
        functools.partial(differ_body, plan, pairwise),
        (part_shape(0), send_shape(0), stat_shape, square_shape(BF16), block_shape),
        (*own_grads, moved_grads, keys, values, e, eb, out, columns),
        [source_scratch, square_scratch, pltpu.VMEM((lanes, 128), F32)],
        vmem_mib=6,
    )
    turned = kernel(
        "turn", turn_body, jax.ShapeDtypeStruct((groups, slots, 2 * lanes), BF16), (eb, yb), []
    )

    stat = stat_own
    for k in range(plan.rounds):
        swap = plan.swap(k)
        stat_came = lax.ppermute(stat, "ctx", swap)
        came = lax.ppermute(send, "ctx", swap)
        merged = call(
            merge_statistics_body,
            stat_shape,
            2,
            10**6,
            in_specs=[VMEM] * 2,
            out_specs=VMEM,
            name=f"statistics{k}",
        )(stat, stat_came)
        if k < plan.rounds - 1:
            outs = (part_shape(k + 1), send_shape(k + 1))
        elif pairwise:
            outs = (jax.ShapeDtypeStruct((2, plan.part_rows, plan.features), BF16),) * 2
        else:
            outs = (jax.ShapeDtypeStruct((2, plan.last_rows, plan.features), BF16),)
        part, send, *_ = call(
            functools.partial(merge_body, plan, k),
            outs,
            4,
            10**8,
            in_specs=[VMEM] * 4,
            out_specs=[VMEM] * len(outs),
            scratch_shapes=[pltpu.VMEM((lanes, 128), F32)],
            name=f"merge{k}",
        )(part, came, stat, stat_came) + (None,) * (2 - len(outs))
        stat = merged
    if pairwise:
        own, away = part, send
        back = lax.ppermute(away, "query", [(0, 1), (1, 0)])

    def gradients(name, first, count, *into):
        return call(
            functools.partial(backward_body, plan, first, count),
            (context_shape, context_shape),
            8,
            4 * 10**9,
            in_specs=[VMEM] * 5 + [HBM] * len(into),
            out_specs=[HBM] * 2,
            scratch_shapes=[
                pltpu.VMEM((lanes, 128), F32),
                pltpu.VMEM((count, slots, width), BF16),
                pltpu.VMEM((count, slots, width), BF16),
                pltpu.SemaphoreType.DMA((2, count)),
            ],
            input_output_aliases={5 + n: n for n in range(len(into))},
            name=name,
        )(stat_own, stat, qb, gb, turned, *into)

    split = (groups + 1) // 2
    grads = gradients("backward0", 0, split)
    key_grad, value_grad = gradients("backward1", split, groups - split, *grads)

    if not pairwise:
        final = lax.all_to_all(part, "query", split_axis=1, concat_axis=2, tiled=True)
        return final[0], final[1], key_grad, value_grad
    whole_rows = jax.ShapeDtypeStruct((plan.part_rows, 2 * plan.features), BF16)
    attn, query_grad = kernel(
        "gather", functools.partial(gather_body, plan), (whole_rows, whole_rows), (own, back), []
    )
    return attn, query_grad, key_grad, value_grad


def solution(mesh):
    placed = (
        P("query", None),
        P("ctx", "query"),
        P("ctx", "query"),
        P("ctx"),
        P(),
        P("ctx"),
        P("query", None),
    )

    return jax.shard_map(
        local,
        mesh=mesh,
        in_specs=placed,
        out_specs=(
            P(("query", "ctx"), None),
            P(("query", "ctx"), None),
            P("ctx", "query"),
            P("ctx", "query"),
        ),
        check_vma=False,
    )
```

```python
import functools
import math

import jax
import jax.numpy as jnp
from jax import lax
from jax.experimental import pallas as pl
from jax.experimental.pallas import tpu as pltpu
from jax.sharding import PartitionSpec as P


F32 = jnp.float32
BF16 = jnp.bfloat16
MIB = 1024 * 1024
LOG2_E = math.log2(math.e)
VMEM = pl.BlockSpec(memory_space=pltpu.VMEM)
HBM = pl.BlockSpec(memory_space=pltpu.HBM)


def call(body, out_shape, vmem_mib, flops, **kwargs):
    return pl.pallas_call(
        body,
        out_shape=out_shape,
        compiler_params=pltpu.CompilerParams(vmem_limit_bytes=vmem_mib * MIB),
        cost_estimate=pl.CostEstimate(flops=flops, bytes_accessed=MIB, transcendentals=0),
        **kwargs,
    )


def nt(a, b):
    return lax.dot_general(a, b, (((1,), (1,)), ((), ())), preferred_element_type=F32)


def nn(a, b):
    return lax.dot_general(a, b, (((1,), (0,)), ((), ())), preferred_element_type=F32)


class Plan:
    def __init__(self, query_states, key_states, level_bias):
        self.query_ways = lax.axis_size("query")
        self.owner_ways = lax.axis_size("ctx")
        self.slots, self.features = key_states.shape
        self.heads = level_bias.shape[1] // self.query_ways
        self.head_size = self.features // self.heads
        self.scale = 1.0 / math.sqrt(self.head_size)
        self.log2_scale = self.scale * LOG2_E
        self.own_rows = query_states.shape[0]
        self.rows = self.own_rows * self.query_ways
        self.part_rows = self.own_rows // self.owner_ways
        self.last_rows = self.part_rows * self.query_ways
        self.group = 2 if self.heads % 2 == 0 and self.rows <= 128 else 1
        self.groups = self.heads // self.group
        self.lanes = self.group * self.rows
        self.rounds = self.owner_ways.bit_length() - 1
        assert 1 << self.rounds == self.owner_ways and self.groups <= 8
        counts = [self.rows]
        for _ in range(self.rounds):
            half = counts[-1] // 2
            counts.append(half if half >= 8 else counts[-1])
        self.counts = counts
        self.packed = None
        if self.rounds and counts[-2] == counts[-1] == 8 and self.rows >> self.rounds == 4 and self.group == 2:
            self.packed = self.rounds - 1

    def split(self, k):
        return k < self.rounds and self.counts[k + 1] < self.counts[k]

    def sent_heads(self, k):
        return self.heads // 2 if k == self.packed else self.heads

    def swapped(self, k):
        return 3 - k if self.rounds >= 3 and k in (1, 2) else k

    def bit(self, k):
        owner = lax.axis_index("ctx")
        return (owner >> jnp.where(owner % 2 == 1, self.swapped(k), k)) & 1

    def swap(self, k):
        return [
            (i, i ^ (1 << (self.swapped(k) if i % 2 else k))) for i in range(self.owner_ways)
        ]

    def keep(self, k):
        return self.bit(k) * self.counts[k + 1] if self.split(k) else 0

    def give(self, k):
        return (1 - self.bit(k)) * self.counts[k + 1] if self.split(k) else 0

    def base(self, k):
        return sum((self.keep(j) for j in range(k)), 0)

    def last_offset(self):
        offset = 0
        for k in range(self.rounds):
            if not self.split(k) and k != self.packed:
                offset = offset + self.bit(k) * (self.rows >> (k + 1))
        return offset


def aligned(x, by):
    return pl.multiple_of(x, by) if by >= 8 and not isinstance(x, int) else x


def halves(first, second, upper):
    top = lax.broadcasted_iota(jnp.int32, first.shape, 0) < 4
    lower_rows = jnp.where(top, first, pltpu.roll(second, 4, 0))
    upper_rows = jnp.where(top, pltpu.roll(first, 4, 0), second)
    return jnp.where(upper == 1, upper_rows, lower_rows)


def copy_all(pairs, semaphores):
    copies = [
        pltpu.make_async_copy(source, target, semaphores.at[n]) for n, (source, target) in enumerate(pairs)
    ]
    for copy in copies:
        copy.start()
    return copies


def columns_at(plan, ref, at):
    return ref.at[:, pl.ds(pl.multiple_of(at * plan.features, 128), plan.features)]


def cut_body(plan, q_ref, g_ref, their_q_ref, their_g_ref, semaphores):
    at = 1 - lax.axis_index("query")
    pairs = [(columns_at(plan, q_ref, at), their_q_ref), (columns_at(plan, g_ref, at), their_g_ref)]
    for copy in copy_all(pairs, semaphores):
        copy.wait()


def load_body(plan, pairwise, *refs):
    count = 6 if pairwise else 4
    ids_hbm, bias_hbm, k_hbm, v_hbm, *rows_hbm = refs[:count]
    k_ref, v_ref, kt_ref, *rows_refs, term_ref, ids_ref, bias_ref, semaphores = refs[count:]
    me = lax.axis_index("query")
    pieces = [slice(j, j + PIECE) for j in range(0, plan.slots, PIECE)]
    parts = [(k_hbm, k_ref, kt_ref, of) for of in pieces] + [(v_hbm, v_ref, None, of) for of in pieces]
    copies = copy_all(
        [
            (ids_hbm, ids_ref),
            (bias_hbm, bias_ref),
            *((source.at[of], target.at[of]) for source, target, _, of in parts),
            *((columns_at(plan, source, me), target) for source, target in zip(rows_hbm, rows_refs)),
        ],
        semaphores,
    )
    for copy in copies[:2]:
        copy.wait()
    ids = ids_ref[...]
    masks = [ids == level for level in range(bias_ref.shape[0])]
    for h in range(plan.heads):
        row = jnp.zeros(ids.shape, F32)
        for level, mask in enumerate(masks):
            row = jnp.where(mask, bias_ref[level, me * plan.heads + h], row)
        term_ref[h : h + 1, :] = row
    for copy, (_, target, turned, of) in zip(copies[2:], parts):
        copy.wait()
        if turned is not None:
            turned[:, of] = target[of].T
    for copy in copies[2 + len(parts) :]:
        copy.wait()


def mask_body(live_ref, term_ref, masked_ref):
    slot = lax.broadcasted_iota(jnp.int32, term_ref.shape, 1)
    masked_ref[...] = jnp.where(slot < live_ref[0], term_ref[...] * LOG2_E, -1e30)


def row_order(plan):
    rows = plan.rows
    place = lax.broadcasted_iota(jnp.int32, (rows, rows), 0)
    column = lax.broadcasted_iota(jnp.int32, (rows, rows), 1)
    inner = place % plan.last_rows
    outer = place // plan.last_rows
    owner = jnp.zeros_like(outer)
    for k in range(plan.rounds):
        bit = (outer >> (plan.rounds - 1 - k)) & 1
        odd = (outer >> (plan.rounds - 1)) & 1
        owner = owner | (bit << jnp.where(odd == 1, plan.swapped(k), k))
    wanted = (
        inner // plan.part_rows * plan.own_rows + owner * plan.part_rows + inner % plan.part_rows
    )
    return (column == wanted).astype(F32).astype(BF16)


def place_rows(plan, own_ref, moved_ref, block_ref, source):
    rows, size = plan.rows, plan.head_size
    width = plan.group * size
    if own_ref is None:
        source[...] = moved_ref[...]
    else:
        source[: plan.own_rows] = own_ref[...]
        source[plan.own_rows :] = moved_ref[...]
    if plan.group > 1:
        block_ref[...] = jnp.zeros_like(block_ref)
    permute = row_order(plan)
    for p in range(plan.groups):
        ordered = nn(permute, source[:, p * width : (p + 1) * width]).astype(BF16)
        for q in range(plan.group):
            block_ref[p, q * rows : (q + 1) * rows, q * size : (q + 1) * size] = ordered[
                :, q * size : (q + 1) * size
            ]


STEP = 16
PIECE = 256
TILE = 256


def pipeline(plan, product, chunk, finish):
    tiles = range(0, plan.slots, TILE)
    for j in tiles:
        product(0, j)
    chunks = range(0, plan.lanes, STEP)
    for p in range(plan.groups):
        pending = [functools.partial(product, p + 1, j) for j in tiles] if p + 1 < plan.groups else []
        if p:
            pending.insert(1, functools.partial(finish, p - 1))
        share = -(-len(pending) // len(chunks)) if pending else 0
        gap = max(1, len(chunks) // max(1, len(pending)))
        for i, r in enumerate(chunks):
            chunk(p, r)
            if i % gap == gap - 1:
                for _ in range(share):
                    if pending:
                        pending.pop(0)()
        for work in pending:
            work()
    finish(plan.groups - 1)


def attend_body(plan, pairwise, *refs):
    own_ref = refs[0] if pairwise else None
    refs = refs[1:] if pairwise else refs
    moved_ref, kt_ref, v_ref, term_ref, eb_ref, out_ref, columns, block_ref, source, scores = refs
    place_rows(plan, own_ref, moved_ref, block_ref, source)
    rows, size, group = plan.rows, plan.head_size, plan.group
    width = group * size
    columns[...] = jnp.zeros_like(columns)

    def product(p, j):
        scores[p % 2, :, j : j + TILE] = nn(block_ref[p], kt_ref[p * width : (p + 1) * width, j : j + TILE])

    def chunk(p, r):
        h = p * group + r // rows
        s = scores[p % 2, r : r + STEP] * plan.log2_scale + term_ref[h : h + 1, :]
        top = jnp.max(s, axis=1, keepdims=True)
        e = jnp.exp2(s - top)
        eb_ref[p, r : r + STEP, :] = e.astype(BF16)
        columns[r : r + STEP, p : p + 1] = top
        columns[r : r + STEP, 8 + p : 9 + p] = jnp.sum(e, axis=1, keepdims=True)

    def finish(p):
        with_values = nn(eb_ref[p], v_ref[:, p * width : (p + 1) * width])
        for q in range(group):
            at, of = slice(q * rows, (q + 1) * rows), slice(q * size, (q + 1) * size)
            out_ref[p * group + q] = with_values[at, of]

    pipeline(plan, product, chunk, finish)


def differ_body(plan, pairwise, *refs):
    own_ref = refs[0] if pairwise else None
    refs = refs[1:] if pairwise else refs
    moved_ref, k_ref, vt_ref, eb_ref, out_ref, columns_ref = refs[:6]
    part_ref, send_ref, stat_ref, yb_ref, block_ref, source, dprobs, columns = refs[6:]
    place_rows(plan, own_ref, moved_ref, block_ref, source)
    rows, size, group = plan.rows, plan.head_size, plan.group
    width = group * size
    columns[...] = columns_ref[...]
    part_ref[0] = out_ref[...]

    def product(p, j):
        dprobs[p % 2, :, j : j + TILE] = nt(block_ref[p], vt_ref[j : j + TILE, p * width : (p + 1) * width])

    def chunk(p, r):
        e = eb_ref[p, r : r + STEP, :].astype(F32)
        d = dprobs[p % 2, r : r + STEP]
        total = columns_ref[r : r + STEP, 8 + p : 9 + p]
        mean = jnp.sum(e * d, axis=1, keepdims=True) / total
        yb_ref[p, r : r + STEP, :] = (e * (d - mean)).astype(BF16)
        columns[r : r + STEP, 16 + p : 17 + p] = mean

    def finish(p):
        both = jnp.concatenate([eb_ref[p], yb_ref[p]], axis=0)
        with_keys = nn(both, k_ref[:, p * width : (p + 1) * width])
        for a in range(2):
            for q in range(group):
                start, of = a * plan.lanes + q * rows, slice(q * size, (q + 1) * size)
                part_ref[1 + a, p * group + q] = with_keys[start : start + rows, of]

    pipeline(plan, product, chunk, finish)
    give(plan, 0, part_ref, send_ref)
    stat_ref[...] = columns[...].T[:24]


def statistics(stat_ref, stat_came_ref):
    top1, total1, mean1 = (stat_ref[8 * t : 8 * t + 8] for t in range(3))
    top2, total2, mean2 = (stat_came_ref[8 * t : 8 * t + 8] for t in range(3))
    top = jnp.maximum(top1, top2)
    f1 = jnp.exp2(top1 - top)
    f2 = jnp.exp2(top2 - top)
    total = f1 * total1 + f2 * total2
    inverse = 1.0 / jnp.where(total > 0.0, total, 1.0)
    w1 = f1 * total1 * inverse
    w2 = f2 * total2 * inverse
    gap = mean1 - mean2
    merged = (top, total, mean1 * w1 + mean2 * w2)
    return merged, (f1, f2, f1 * w2 * gap, -f2 * w1 * gap, inverse)


def merge_statistics_body(stat_ref, stat_came_ref, stat_new_ref):
    merged, _ = statistics(stat_ref, stat_came_ref)
    for t in range(3):
        stat_new_ref[8 * t : 8 * t + 8] = merged[t]


def merge_body(plan, k, part_ref, came_ref, stat_ref, stat_came_ref, *refs):
    last = k == plan.rounds - 1
    if last:
        own_ref, away_ref, table = refs if len(refs) == 3 else (None, *refs)
    else:
        part_new_ref, send_ref, table = refs
    _, factors = statistics(stat_ref, stat_came_ref)
    rest = jnp.zeros((128 - 40, plan.lanes), F32)
    table[...] = jnp.concatenate([*factors, rest], axis=0).T
    count = plan.counts[k + 1]
    kept = pl.ds(aligned(plan.keep(k), count), count)
    base = plan.base(k + 1)
    rows_of = [pl.ds(aligned(q * plan.rows + base, count), count) for q in range(plan.group)]
    packed = k == plan.packed
    bit = plan.bit(k)
    if packed:
        joined = halves(table[rows_of[0], :], table[rows_of[1], :], bit)
    for n in range(plan.sent_heads(k)):
        if packed:
            p = n
            mine = [halves(part_ref[a, 2 * n], part_ref[a, 2 * n + 1], bit) for a in range(3)]
            rows = joined
        else:
            p = n // plan.group
            mine = [part_ref[a, n, kept, :] for a in range(3)]
            rows = table[rows_of[n % plan.group], :]
        col = lambda t: rows[:, 8 * t + p : 8 * t + p + 1]
        out1, key1, dif1 = mine
        out2, key2, dif2 = (came_ref[a, n].astype(F32) for a in range(3))
        c1, c2 = col(0), col(1)
        out = c1 * out1 + c2 * out2
        dif = c1 * dif1 + c2 * dif2 + col(2) * key1 + col(3) * key2
        if not last:
            part_new_ref[0, n] = out
            part_new_ref[1, n] = c1 * key1 + c2 * key2
            part_new_ref[2, n] = dif
            continue
        share = col(4)
        for a, x in ((0, out * share), (1, dif * (share * plan.scale))):
            offset = plan.last_offset()
            if not isinstance(offset, int):
                x = pltpu.roll(x, (count - offset) % count, 0)
            for h, start in ((2 * n, 0), (2 * n + 1, 4)) if packed else ((n, 0),):
                of = slice(h * plan.head_size, (h + 1) * plan.head_size)
                middle, end = start + plan.part_rows, start + plan.last_rows
                if own_ref is not None:
                    own_ref[a, :, of] = x[start:middle].astype(BF16)
                    away_ref[a, :, of] = x[middle:end].astype(BF16)
                else:
                    away_ref[a, :, of] = x[start:end].astype(BF16)
    if not last:
        give(plan, k + 1, part_new_ref, send_ref)


def give(plan, k, part_ref, send_ref):
    if k == plan.packed:
        for a in range(3):
            for n in range(plan.heads // 2):
                x = halves(part_ref[a, 2 * n], part_ref[a, 2 * n + 1], 1 - plan.bit(k))
                send_ref[a, n] = x.astype(BF16)
        return
    count = plan.counts[k + 1]
    gone = pl.ds(aligned(plan.give(k), count), count)
    for a in range(3):
        for h in range(plan.heads):
            send_ref[a, h] = part_ref[a, h, gone, :].astype(BF16)


def gather_body(plan, own_ref, back_ref, attn_ref, dq_ref):
    me = lax.axis_index("query")
    for a, out_ref in ((0, attn_ref), (1, dq_ref)):
        for at, ref in ((me, own_ref), (1 - me, back_ref)):
            start = pl.multiple_of(at * plan.features, 128)
            out_ref[:, pl.ds(start, plan.features)] = ref[a]


def turn_body(eb_ref, yb_ref, turned_ref):
    lanes = eb_ref.shape[1]
    for p in range(eb_ref.shape[0]):
        turned_ref[p, :, :lanes] = eb_ref[p].T
        turned_ref[p, :, lanes:] = yb_ref[p].T


def backward_body(plan, first, count, stat_ref, stat_all_ref, qb_ref, gb_ref, turned_ref, *refs):
    dk_ref, dv_ref, table, dk, dv, semaphores = refs[-6:]
    lanes = plan.lanes
    width = dk.shape[2]
    total = stat_all_ref[8:16]
    inverse = 1.0 / jnp.where(total > 0.0, total, 1.0)
    f = jnp.exp2(stat_ref[0:8] - stat_all_ref[0:8]) * inverse
    c = f * (stat_ref[16:24] - stat_all_ref[16:24])
    rest = jnp.zeros((128 - 24, lanes), F32)
    table[...] = jnp.concatenate([f, f * plan.scale, c * plan.scale, rest], axis=0).T
    copies = []
    for p in range(first, first + count):
        queries = qb_ref[p].astype(F32)
        wv = (gb_ref[p].astype(F32) * table[:, p : p + 1]).astype(BF16)
        wc = (queries * table[:, 16 + p : 17 + p]).astype(BF16)
        wf = (queries * table[:, 8 + p : 9 + p]).astype(BF16)
        for n, (buffer, target) in enumerate(((dk, dk_ref), (dv, dv_ref))):
            if n == 0:
                buffer[p - first] = nn(turned_ref[p], jnp.concatenate([wc, wf], axis=0)).astype(BF16)
            else:
                buffer[p - first] = nn(turned_ref[p, :, :lanes], wv).astype(BF16)
            copy = pltpu.make_async_copy(
                buffer.at[p - first], target.at[:, p * width : (p + 1) * width], semaphores.at[n, p - first]
            )
            copy.start()
            copies.append(copy)
    for copy in copies:
        copy.wait()


def local(query_states, key_states, value_states, level_ids, level_bias, live_counts, out_grad):
    plan = Plan(query_states, key_states, level_bias)
    size, slots, lanes, groups, heads = plan.head_size, plan.slots, plan.lanes, plan.groups, plan.heads
    width = plan.group * size
    pairwise = plan.query_ways == 2
    own_shape = jax.ShapeDtypeStruct((plan.own_rows, plan.features), BF16)
    pairwise = plan.query_ways == 2
    in_hbm = lambda arrays: [pltpu.with_memory_space_constraint(x, pltpu.HBM) for x in arrays]
    if pairwise:
        their_queries, their_grads = call(
            functools.partial(cut_body, plan),
            [own_shape] * 2,
            2,
            10**6,
            in_specs=[HBM] * 2,
            out_specs=[VMEM] * 2,
            scratch_shapes=[pltpu.SemaphoreType.DMA((2,))],
            name="cut",
        )(*in_hbm([query_states, out_grad]))
        moved_queries = lax.ppermute(their_queries, "query", [(0, 1), (1, 0)])
        moved_grads = lax.ppermute(their_grads, "query", [(0, 1), (1, 0)])
    else:
        moved_queries, moved_grads = (
            lax.all_to_all(x, "query", split_axis=1, concat_axis=0, tiled=True)
            for x in (query_states, out_grad)
        )

    stat_shape = jax.ShapeDtypeStruct((24, lanes), F32)
    block_shape = jax.ShapeDtypeStruct((groups, lanes, width), BF16)
    square_shape = lambda dtype: jax.ShapeDtypeStruct((groups, lanes, slots), dtype)
    part_shape = lambda k: jax.ShapeDtypeStruct((3, heads, plan.counts[k], size), F32)
    send_shape = lambda k: jax.ShapeDtypeStruct(
        (3, plan.sent_heads(k), plan.counts[k + 1], size), BF16
    )
    context_shape = jax.ShapeDtypeStruct(key_states.shape, BF16)
    columns_shape = jax.ShapeDtypeStruct((lanes, 128), F32)
    source_scratch = pltpu.VMEM((plan.rows, plan.features), BF16)
    square_scratch = pltpu.VMEM((2, lanes, slots), F32)

    def kernel(name, body, outs, ins, scratch, vmem_mib=4, flops=10**9):
        single = not isinstance(outs, (tuple, list))
        return call(
            body,
            outs,
            vmem_mib,
            flops,
            in_specs=[VMEM] * len(ins),
            out_specs=VMEM if single else [VMEM] * len(outs),
            scratch_shapes=scratch,
            name=name,
        )(*ins)

    from_hbm = [level_ids.reshape(1, slots), level_bias, key_states, value_states]
    from_hbm += [query_states, out_grad] if pairwise else []
    own_shapes = [own_shape] * 2 if pairwise else []
    turned_shape = jax.ShapeDtypeStruct((plan.features, slots), BF16)
    term_shape = jax.ShapeDtypeStruct((heads, slots), F32)
    keys, values, keys_turned, *own, term = call(
        functools.partial(load_body, plan, pairwise),
        [context_shape] * 2 + [turned_shape] + own_shapes + [term_shape],
        4,
        10**9,
        in_specs=[HBM] * len(from_hbm),
        out_specs=[VMEM] * (4 + len(own_shapes)),
        scratch_shapes=[
            pltpu.VMEM((1, slots), jnp.int32),
            pltpu.SMEM(level_bias.shape, F32),
            pltpu.SemaphoreType.DMA((len(from_hbm) - 2 + 2 * slots // PIECE,)),
        ],
        name="load",
    )(*in_hbm(from_hbm))
    term = call(
        mask_body,
        term_shape,
        2,
        10**6,
        in_specs=[pl.BlockSpec(memory_space=pltpu.SMEM), VMEM],
        out_specs=VMEM,
        name="mask",
    )(live_counts, term)
    own_queries, own_grads = ([own[0]], [own[1]]) if pairwise else ([], [])
    eb, out, columns, qb = kernel(
        "attend",
        functools.partial(attend_body, plan, pairwise),
        (
            square_shape(BF16),
            jax.ShapeDtypeStruct((heads, plan.rows, size), F32),
            columns_shape,
            block_shape,
        ),
        (*own_queries, moved_queries, keys_turned, values, term),
        [source_scratch, square_scratch],
        vmem_mib=6,
    )
    part, send, stat_own, yb, gb = kernel(
        "differ",
        functools.partial(differ_body, plan, pairwise),
        (part_shape(0), send_shape(0), stat_shape, square_shape(BF16), block_shape),
        (*own_grads, moved_grads, keys, values, eb, out, columns),
        [source_scratch, square_scratch, pltpu.VMEM((lanes, 128), F32)],
        vmem_mib=6,
    )
    turned = kernel(
        "turn", turn_body, jax.ShapeDtypeStruct((groups, slots, 2 * lanes), BF16), (eb, yb), []
    )

    stat = stat_own
    for k in range(plan.rounds):
        swap = plan.swap(k)
        stat_came = lax.ppermute(stat, "ctx", swap)
        came = lax.ppermute(send, "ctx", swap)
        merged = call(
            merge_statistics_body,
            stat_shape,
            2,
            10**6,
            in_specs=[VMEM] * 2,
            out_specs=VMEM,
            name=f"statistics{k}",
        )(stat, stat_came)
        if k < plan.rounds - 1:
            outs = (part_shape(k + 1), send_shape(k + 1))
        elif pairwise:
            outs = (jax.ShapeDtypeStruct((2, plan.part_rows, plan.features), BF16),) * 2
        else:
            outs = (jax.ShapeDtypeStruct((2, plan.last_rows, plan.features), BF16),)
        part, send, *_ = call(
            functools.partial(merge_body, plan, k),
            outs,
            4,
            10**8,
            in_specs=[VMEM] * 4,
            out_specs=[VMEM] * len(outs),
            scratch_shapes=[pltpu.VMEM((lanes, 128), F32)],
            name=f"merge{k}",
        )(part, came, stat, stat_came) + (None,) * (2 - len(outs))
        stat = merged
    if pairwise:
        own, away = part, send
        back = lax.ppermute(away, "query", [(0, 1), (1, 0)])

    def gradients(name, first, count, *into):
        return call(
            functools.partial(backward_body, plan, first, count),
            (context_shape, context_shape),
            8,
            4 * 10**9,
            in_specs=[VMEM] * 5 + [HBM] * len(into),
            out_specs=[HBM] * 2,
            scratch_shapes=[
                pltpu.VMEM((lanes, 128), F32),
                pltpu.VMEM((count, slots, width), BF16),
                pltpu.VMEM((count, slots, width), BF16),
                pltpu.SemaphoreType.DMA((2, count)),
            ],
            input_output_aliases={5 + n: n for n in range(len(into))},
            name=name,
        )(stat_own, stat, qb, gb, turned, *into)

    split = (groups + 1) // 2
    grads = gradients("backward0", 0, split)
    key_grad, value_grad = gradients("backward1", split, groups - split, *grads)

    if not pairwise:
        final = lax.all_to_all(part, "query", split_axis=1, concat_axis=2, tiled=True)
        return final[0], final[1], key_grad, value_grad
    whole_rows = jax.ShapeDtypeStruct((plan.part_rows, 2 * plan.features), BF16)
    attn, query_grad = kernel(
        "gather", functools.partial(gather_body, plan), (whole_rows, whole_rows), (own, back), []
    )
    return attn, query_grad, key_grad, value_grad


def solution(mesh):
    placed = (
        P("query", None),
        P("ctx", "query"),
        P("ctx", "query"),
        P("ctx"),
        P(),
        P("ctx"),
        P("query", None),
    )

    return jax.shard_map(
        local,
        mesh=mesh,
        in_specs=placed,
        out_specs=(
            P(("query", "ctx"), None),
            P(("query", "ctx"), None),
            P("ctx", "query"),
            P("ctx", "query"),
        ),
        check_vma=False,
    )
```
